256 devices in a mesh: feat: 64 (over z, y, x_hi), row: 2 (over x_lo), col: 2 (over core).
Axes of the slice: x: 4 (x_hi: 2, x_lo: 2; x = x_hi * 2 + x_lo), y: 4, z: 8, core: 2. Of those that a mesh axis runs over, the one named last changes fastest.
Arguments:
- local_x: float32 [4, 256, 256], P(('row', 'col'), 'feat'), may hold values from -4 to 4
- dual_var: float32 [4, 256, 256], P(('row', 'col'), 'feat'), may hold values from -2 to 2
- consensus_old: float32 [256, 256], P('feat'), may hold values from -4 to 4
- blocks_data: bfloat16 [4, 256, 512, 256], P(('row', 'col'), 'feat'), may hold values from -0.375 to 0.375
- row_index: int32 [4, 256, 512], P(('row', 'col'), 'feat'), may hold values from 0 to 16383, as said below
- labels: int32 [4, 16384], P(('row', 'col')), may hold values 0 or 1
Outputs:
- solved_x: float32 [4, 256, 256], P(('row', 'col'), 'feat')
- dual_new: float32 [4, 256, 256], P(('row', 'col'), 'feat')
- consensus: float32 [256, 256], P('feat')
- norms: float32 [2], replicated
The draws below stay inside these ranges and needn't reach their ends.
Inputs may be any that keep to these rules, and one draw needn't show every extreme that they name: `row_index`: the 512 rows of one block are distinct samples of its shard; a sample may appear in no block or in several.
All inputs are finite; a program needn't handle non-finite values. No bound on the sum of `labels` on one device may be relied on, other than what follows from the above.
Results may differ from the reference program's by a relative error of at most 0.0019.
Values sent between devices are 32-bit elements; how exact they have to be, the bound alone decides.
No kernel may reach another device: no remote copies, remote signals or barrier semaphores. Data moves between devices by JAX's collectives and lax.ppermute only.
A program may use at most 64 MiB of HBM per device.

```python
import jax
import jax.numpy as jnp
from jax import lax

BLOCK_COLS = 256
BLOCK_ROWS = 512
SAMPLES_DEV = 16384
NEWTON_STEPS = 2
CG_STEPS = 3
SHARDS = 4
BLOCKS = 256


def draw_row_index(key, part):
    keys = jax.random.split(jax.random.fold_in(key, 17), SHARDS * BLOCKS)

    def one_block(block_key):
        return jax.random.permutation(block_key, SAMPLES_DEV)[:BLOCK_ROWS].astype(jnp.int32)
    picks = lax.map(one_block, keys)
    return picks.reshape(SHARDS, BLOCKS, BLOCK_ROWS).astype(jnp.int32)


def draw_dual_var(key, part):
    inner = jax.random.fold_in(key, 29)
    position = jnp.arange(BLOCKS, dtype=jnp.float32) / jnp.float32(max(BLOCKS - 1, 1))
    scales = 0.05 * jnp.power(10.0, position)
    raw = jax.random.normal(inner, (SHARDS, BLOCKS, BLOCK_COLS), jnp.float32)
    values = raw * scales[None, :, None]
    return jnp.clip(values, -2.0, 2.0).astype(jnp.float32)


def with_ends(drawn, key, low, largest):
    longest = drawn.shape.index(max(drawn.shape))
    spots = []
    for shift in (0, 1):
        where = [jax.random.randint(jax.random.fold_in(key, axis), (), 0, length) for axis, length in enumerate(drawn.shape)]
        where[longest] = (where[longest] + shift) % drawn.shape[longest]
        spots.append(tuple(where))
    return drawn.at[spots[0]].set(low).at[spots[1]].set(largest)


def levels(rng, extent, cuts, smallest, high):
    def one(dim, shards_of):
        draws = jax.random.uniform(jax.random.fold_in(jax.random.fold_in(rng, 6), dim), (shards_of,), jnp.float32, smallest / len(cuts), high / len(cuts))
        return jnp.repeat(jnp.exp(draws), extent[dim] // shards_of).reshape((-1,) + (1,) * (len(extent) - dim - 1))

    gain = one(*cuts[0])
    for cut in cuts[1:]:
        gain = gain * one(*cut)
    return gain


def bell_draw(key, extent, deviation, limit, cuts=(), kind=jnp.bfloat16):
    loudness = levels(key, extent, cuts, -0.22, 0.18) if cuts else 1.0
    drawn = jax.random.normal(key, extent, jnp.float32) * deviation * loudness
    return jnp.minimum(jnp.maximum(drawn, -limit), limit).astype(kind)


def setup_inputs(seed: int = 0) -> dict:
    arg_keys = jax.random.split(jax.random.key(seed), 7)
    local_x = bell_draw(arg_keys[0], (SHARDS, BLOCKS, BLOCK_COLS), 0.5, 4.0, ((0, 4), (1, 64)), jnp.float32)
    dual_var = draw_dual_var(jax.random.fold_in(arg_keys[6], 71), 0)
    consensus_old = bell_draw(arg_keys[2], (BLOCKS, BLOCK_COLS), 0.5, 4.0, ((0, 64),), jnp.float32)
    blocks_data = bell_draw(arg_keys[3], (SHARDS, BLOCKS, BLOCK_ROWS, BLOCK_COLS), BLOCK_COLS ** -0.5, 0.375, ((0, 4), (1, 64)))
    row_index = draw_row_index(jax.random.fold_in(arg_keys[6], 71), 0)
    labels = with_ends((jax.random.randint(arg_keys[5], (SHARDS, SAMPLES_DEV), 0, 2) < 1).astype(jnp.int32), jax.random.fold_in(arg_keys[5], 1), 0, 1)
    return {"local_x": local_x, "dual_var": dual_var, "consensus_old": consensus_old, "blocks_data": blocks_data, "row_index": row_index, "labels": labels}


penalty = 1.0
damping = 0.5
threshold = 0.05

def conjugate_solve(hessian, gradient):
    delta = jnp.zeros_like(gradient)
    residual = gradient
    direction = gradient
    power = lax.optimization_barrier(jnp.sum(residual * residual, axis=1))
    for cg_step in range(CG_STEPS):
        image = jnp.einsum('bkl,bl->bk', hessian, direction, precision=lax.Precision.HIGHEST)
        alpha = power / lax.optimization_barrier(jnp.sum(direction * image, axis=1))
        delta = delta + alpha[:, None] * direction
        residual = residual - alpha[:, None] * image
        power_next = lax.optimization_barrier(jnp.sum(residual * residual, axis=1))
        direction = residual + (power_next / power)[:, None] * direction
        power = power_next
    return delta

def newton_solve(iterate, blocks_data, row_index, labels, target):
    targets = labels.astype(jnp.float32)
    data_wide = blocks_data.astype(jnp.float32)
    flat_index = row_index.reshape(-1)
    identity = jnp.eye(iterate.shape[1], dtype=jnp.float32)
    for newton_step in range(NEWTON_STEPS):
        rounded = lax.optimization_barrier(iterate.astype(jnp.bfloat16)).astype(jnp.float32)
        partial_value = jnp.einsum('brk,bk->br', data_wide, rounded, precision=lax.Precision.HIGHEST)
        margins = jax.ops.segment_sum(partial_value.reshape(-1), flat_index, num_segments=SAMPLES_DEV)
        prob = jax.nn.sigmoid(margins)
        misfit = prob - targets
        weights = prob * (1.0 - prob)
        misfit_rows = lax.optimization_barrier(misfit[row_index].astype(jnp.bfloat16)).astype(jnp.float32)
        gradient = jnp.einsum('brk,br->bk', data_wide, misfit_rows, precision=lax.Precision.HIGHEST)
        gradient = gradient + penalty * (iterate - target)
        weighted = lax.optimization_barrier((data_wide * weights[row_index][:, :, None]).astype(jnp.bfloat16)).astype(jnp.float32)
        hessian = jnp.einsum('brk,brl->bkl', data_wide, weighted, precision=lax.Precision.HIGHEST) + penalty * identity
        delta = conjugate_solve(hessian, gradient)
        iterate = iterate - damping * delta
    return iterate

def reference(local_x, dual_var, consensus_old, blocks_data, row_index, labels):
    shards = jnp.float32(local_x.shape[0])

    def one_shard(items):
        return newton_solve(items[0], items[1], items[2], items[3], consensus_old - items[4])
    solved = lax.map(one_shard, (local_x, blocks_data, row_index, labels, dual_var))
    averaged = lax.optimization_barrier(jnp.sum(solved + dual_var, axis=0)) / shards
    consensus = jnp.sign(averaged) * jnp.maximum(jnp.abs(averaged) - threshold, 0.0)
    dual_new = dual_var + solved - consensus
    primal = jnp.sqrt(jnp.sum((solved - consensus) ** 2))
    dual_norm = penalty * jnp.sqrt(shards * jnp.sum((consensus - consensus_old) ** 2))
    return (solved, dual_new, consensus, jnp.stack([primal, dual_norm]))
```

```python
import jax
import jax.numpy as jnp
from jax import lax
from jax.experimental import pallas as pl
from jax.experimental.pallas import tpu as pltpu
from jax.sharding import Mesh
from jax.sharding import PartitionSpec as P

CG_STEPS = 3
FEAT = ("feat_0", "feat_1", "feat_2")
SHARD = ("row", "col")
LANES = 128
HIGH = 64
LOW = 256
INTERPRET = False

penalty = 1.0
damping = 0.5
threshold = 0.05


def call(kernel, *outs):
    return pl.pallas_call(
        kernel,
        out_shape=tuple(jax.ShapeDtypeStruct(shape, jnp.float32) for shape in outs),
        interpret=INTERPRET,
    )


def dot(a, b, dims):
    return lax.dot_general(a, b, (dims, ((), ())), preferred_element_type=jnp.float32)


NN = ((1,), (0,))
NT = ((1,), (1,))


def three_parts(x):
    first = x.astype(jnp.bfloat16).astype(jnp.float32)
    rest = x - first
    second = rest.astype(jnp.bfloat16).astype(jnp.float32)
    return first, second, rest - second


def low_hot(index):
    low = (index & 127) | ((index >> 13) << 7)
    places = lax.broadcasted_iota(jnp.int32, (LOW, index.shape[1]), 0)
    return jnp.where(places == low, 1.0, 0.0).astype(jnp.bfloat16)


def high_mask(index):
    high = (index >> 7) & (HIGH - 1)
    places = lax.broadcasted_iota(jnp.int32, (HIGH, index.shape[1]), 0)
    return places == high


def as_table(lines):
    return jnp.concatenate([lines[:HIGH], lines[HIGH:]], axis=1)


def scattered(x, blk_ref, hots, masks, out_ref):
    rounded = x.astype(jnp.bfloat16)
    table = None
    for b, (hot, mask) in enumerate(zip(hots, masks)):
        partial = dot(rounded, blk_ref[b], NT)[b : b + 1]
        parts = [jnp.where(mask, part, 0.0) for part in three_parts(partial)]
        spread = jnp.concatenate(parts, axis=0).astype(jnp.bfloat16)
        added = dot(spread, hot, NT)
        table = added if table is None else table + added
    table = table[:HIGH] + table[HIGH : 2 * HIGH] + table[2 * HIGH :]
    out_ref[:HIGH, :] = table[:, :LANES]
    out_ref[HIGH:, :] = table[:, LANES:]


def newton_step(x, target, margins, labels, blk_ref, hots, masks):
    blocks, size = x.shape
    parts = three_parts(as_table(margins)) + (as_table(labels.astype(jnp.float32)),)
    tables = jnp.concatenate(parts, axis=0).astype(jnp.bfloat16)
    rows = lax.broadcasted_iota(jnp.int32, (size, size), 0)
    cols = lax.broadcasted_iota(jnp.int32, (size, size), 1)
    identity = jnp.where(rows == cols, 1.0, 0.0)
    gradients = []
    hessians = []
    for b, (hot, mask) in enumerate(zip(hots, masks)):
        block = blk_ref[b]
        found = dot(tables, hot, NN)
        margin = found[:HIGH] + found[HIGH : 2 * HIGH] + found[2 * HIGH : 3 * HIGH]
        margin = jnp.sum(jnp.where(mask, margin, 0.0), axis=0, keepdims=True)
        label = jnp.sum(jnp.where(mask, found[3 * HIGH :], 0.0), axis=0, keepdims=True)
        prob = 1.0 / (1.0 + jnp.exp(-margin))
        misfit = (prob - label).astype(jnp.bfloat16)
        weight = prob * (1.0 - prob)
        gradients.append(dot(misfit, block, NN))
        turned = dot(identity.astype(jnp.bfloat16), block, NT)
        weighted = (turned * weight).astype(jnp.bfloat16)
        hessians.append(dot(weighted, block, NN) + penalty * identity)
    gradient = jnp.concatenate(gradients, axis=0) + penalty * (x - target)
    delta = jnp.zeros_like(gradient)
    residual = gradient
    direction = gradient
    power = jnp.sum(residual * residual, axis=1, keepdims=True)
    for cg_step in range(CG_STEPS):
        column = jnp.transpose(jnp.concatenate([direction, direction], axis=0))
        image = jnp.concatenate(
            [
                jnp.sum(hessians[b] * column[:, b : b + 1], axis=0, keepdims=True)
                for b in range(blocks)
            ],
            axis=0,
        )
        alpha = power / jnp.sum(direction * image, axis=1, keepdims=True)
        delta = delta + alpha * direction
        residual = residual - alpha * image
        power_next = jnp.sum(residual * residual, axis=1, keepdims=True)
        direction = residual + (power_next / power) * direction
        power = power_next
    return x - damping * delta


def hot_rows(idx_ref):
    rows = [idx_ref[b : b + 1, :] for b in range(idx_ref.shape[0])]
    return [low_hot(row) for row in rows], [high_mask(row) for row in rows]


def first_kernel(x_ref, blk_ref, idx_ref, out_ref):
    hots, masks = hot_rows(idx_ref)
    scattered(x_ref[...], blk_ref, hots, masks, out_ref)


def middle_kernel(x_ref, dual_ref, old_ref, margin_ref, label_ref, blk_ref, idx_ref, x_out, out_ref):
    hots, masks = hot_rows(idx_ref)
    target = old_ref[...] - dual_ref[...]
    x = newton_step(x_ref[...], target, margin_ref[...], label_ref[...], blk_ref, hots, masks)
    x_out[...] = x
    scattered(x, blk_ref, hots, masks, out_ref)


def last_kernel(x_ref, dual_ref, old_ref, margin_ref, label_ref, blk_ref, idx_ref, x_out, both_ref):
    hots, masks = hot_rows(idx_ref)
    dual = dual_ref[...]
    target = old_ref[...] - dual
    x = newton_step(x_ref[...], target, margin_ref[...], label_ref[...], blk_ref, hots, masks)
    x_out[...] = x
    both = jnp.concatenate([x, dual], axis=0)
    for shard in range(both_ref.shape[0]):
        both_ref[shard] = both


def consensus_kernel(both_ref, x_ref, dual_ref, old_ref, cons_ref, dual_out, sums_ref):
    shards, lines, size = both_ref.shape
    blocks = lines // 2
    solved = [both_ref[i][:blocks] for i in range(shards)]
    total = solved[0] + both_ref[0][blocks:]
    for i in range(1, shards):
        total = total + (solved[i] + both_ref[i][blocks:])
    averaged = total / float(shards)
    cut = jnp.maximum(jnp.abs(averaged) - threshold, 0.0)
    consensus = jnp.where(averaged < 0.0, -cut, cut)
    cons_ref[...] = consensus
    dual_out[...] = dual_ref[...] + x_ref[...] - consensus
    primal = jnp.zeros_like(consensus)
    for i in range(shards):
        primal = primal + (solved[i] - consensus) ** 2
    change = (consensus - old_ref[...]) ** 2
    primal = jnp.sum(jnp.sum(primal, axis=1, keepdims=True), axis=0, keepdims=True)
    change = jnp.sum(jnp.sum(change, axis=1, keepdims=True), axis=0, keepdims=True)
    lane = lax.broadcasted_iota(jnp.int32, (1, LANES), 1)
    sums = jnp.where(lane == 0, primal, jnp.where(lane == 1, float(shards) * change, 0.0))
    sums_ref[...] = jnp.broadcast_to(sums, sums_ref.shape)


def exchanged(x, axis):
    return lax.all_to_all(x, axis, 0, 0, tiled=True)


def total_of(lines):
    size = lax.axis_size(FEAT)
    parts = exchanged(lines.reshape(size, -1, LANES), FEAT)
    own = jnp.sum(parts, axis=0)
    whole = exchanged(jnp.broadcast_to(own[None], parts.shape), FEAT)
    return whole.reshape(lines.shape)


def local(local_x, dual_var, consensus_old, blocks_data, row_index, labels):
    x = local_x[0]
    dual = dual_var[0]
    blocks = blocks_data[0]
    index = row_index[0]
    marks = labels.reshape(-1, LANES)
    lines = marks.shape
    feats = lax.axis_size(FEAT)
    shards = lax.axis_size(SHARD)
    (terms,) = call(first_kernel, lines)(x, blocks, index)
    margins = total_of(terms)
    x, terms = call(middle_kernel, x.shape, lines)(
        x, dual, consensus_old, margins, marks, blocks, index
    )
    margins = total_of(terms)
    x, both = call(last_kernel, x.shape, (shards, 2 * x.shape[0], x.shape[1]))(
        x, dual, consensus_old, margins, marks, blocks, index
    )
    both = exchanged(both, SHARD)
    consensus, dual_next, sums = call(consensus_kernel, x.shape, x.shape, (feats, LANES))(
        both, x, dual, consensus_old
    )
    sums = jnp.sum(exchanged(sums.reshape(feats, 1, LANES), FEAT), axis=(0, 1))
    norms = jnp.sqrt(sums[:2]) * jnp.array([1.0, penalty], jnp.float32)
    return (x[None], dual_next[None], consensus, norms)


def solution(mesh):
    if mesh.shape["feat"] == 64:
        feat = (8, 4, 2)
    else:
        feat = (mesh.shape["feat"], 1, 1)
    torus = Mesh(
        mesh.devices.reshape(*feat, mesh.shape["row"], mesh.shape["col"]), FEAT + SHARD
    )
    placed = (
        P(SHARD, FEAT, None),
        P(SHARD, FEAT, None),
        P(FEAT, None),
        P(SHARD, FEAT, None, None),
        P(SHARD, FEAT, None),
        P(SHARD, None),
    )
    return jax.shard_map(
        local,
        mesh=torus,
        in_specs=placed,
        out_specs=(P(SHARD, FEAT, None), P(SHARD, FEAT, None), P(FEAT, None), P()),
        check_vma=False,
    )
```

```python
import jax
import jax.numpy as jnp
from jax import lax
from jax.experimental import pallas as pl
from jax.experimental.pallas import tpu as pltpu
from jax.sharding import Mesh
from jax.sharding import PartitionSpec as P

CG_STEPS = 3
FEAT = ("feat_0", "feat_1", "feat_2")
SHARD = ("row", "col")
NEAR = ("feat_2", "row", "col")
FAR = ("feat_0", "feat_1")
LANES = 128
HIGH = 64
LOW = 256
SHARDS = 4
INTERPRET = False

penalty = 1.0
damping = 0.5
threshold = 0.05


def in_vmem(*args):
    if INTERPRET:
        return args
    return [pltpu.with_memory_space_constraint(arg, pltpu.VMEM) for arg in args]


def call(kernel, *outs):
    if INTERPRET:
        shapes = tuple(jax.ShapeDtypeStruct(shape, jnp.float32) for shape in outs)
    else:
        shapes = tuple(pltpu.VMEM(shape, jnp.float32) for shape in outs)
    return pl.pallas_call(kernel, out_shape=shapes, interpret=INTERPRET)


def dot(a, b, dims):
    return lax.dot_general(a, b, (dims, ((), ())), preferred_element_type=jnp.float32)


NN = ((1,), (0,))
NT = ((1,), (1,))


def three_parts(x):
    first = x.astype(jnp.bfloat16).astype(jnp.float32)
    rest = x - first
    second = rest.astype(jnp.bfloat16).astype(jnp.float32)
    return first, second, rest - second


def low_hot(index):
    low = (index & 127) | ((index >> 13) << 7)
    places = lax.broadcasted_iota(jnp.int32, (LOW, index.shape[1]), 0)
    return jnp.where(places == low, 1.0, 0.0).astype(jnp.bfloat16)


def high_mask(index):
    high = (index >> 7) & (HIGH - 1)
    places = lax.broadcasted_iota(jnp.int32, (HIGH, index.shape[1]), 0)
    return places == high


def as_table(lines):
    return jnp.concatenate([lines[:HIGH], lines[HIGH:]], axis=1)


def scattered(x, blk_ref, hots, masks, out_ref):
    rounded = x.astype(jnp.bfloat16)
    table = None
    for b, (hot, mask) in enumerate(zip(hots, masks)):
        partial = dot(rounded, blk_ref[b], NT)[b : b + 1]
        parts = [jnp.where(mask, part, 0.0) for part in three_parts(partial)]
        spread = jnp.concatenate(parts, axis=0).astype(jnp.bfloat16)
        added = dot(spread, hot, NT)
        table = added if table is None else table + added
    table = table[:HIGH] + table[HIGH : 2 * HIGH] + table[2 * HIGH :]
    out_ref[:HIGH, :] = table[:, :LANES]
    out_ref[HIGH:, :] = table[:, LANES:]


def newton_step(x, target, margins, labels, blk_ref, hots, masks):
    blocks, size = x.shape
    parts = three_parts(as_table(margins)) + (as_table(labels.astype(jnp.float32)),)
    tables = jnp.concatenate(parts, axis=0).astype(jnp.bfloat16)
    rows = lax.broadcasted_iota(jnp.int32, (size, size), 0)
    cols = lax.broadcasted_iota(jnp.int32, (size, size), 1)
    identity = jnp.where(rows == cols, 1.0, 0.0)
    gradients = []
    hessians = []
    for b, (hot, mask) in enumerate(zip(hots, masks)):
        block = blk_ref[b]
        found = dot(tables, hot, NN)
        margin = found[:HIGH] + found[HIGH : 2 * HIGH] + found[2 * HIGH : 3 * HIGH]
        margin = jnp.sum(jnp.where(mask, margin, 0.0), axis=0, keepdims=True)
        label = jnp.sum(jnp.where(mask, found[3 * HIGH :], 0.0), axis=0, keepdims=True)
        prob = 1.0 / (1.0 + jnp.exp(-margin))
        misfit = (prob - label).astype(jnp.bfloat16)
        weight = prob * (1.0 - prob)
        gradients.append(dot(misfit, block, NN))
        turned = dot(identity.astype(jnp.bfloat16), block, NT)
        weighted = (turned * weight).astype(jnp.bfloat16)
        hessians.append(dot(weighted, block, NN) + penalty * identity)
    gradient = jnp.concatenate(gradients, axis=0) + penalty * (x - target)
    delta = jnp.zeros_like(gradient)
    residual = gradient
    direction = gradient
    power = jnp.sum(residual * residual, axis=1, keepdims=True)
    for cg_step in range(CG_STEPS):
        column = jnp.transpose(jnp.concatenate([direction, direction], axis=0))
        image = jnp.concatenate(
            [
                jnp.sum(hessians[b] * column[:, b : b + 1], axis=0, keepdims=True)
                for b in range(blocks)
            ],
            axis=0,
        )
        alpha = power / jnp.sum(direction * image, axis=1, keepdims=True)
        delta = delta + alpha * direction
        residual = residual - alpha * image
        power_next = jnp.sum(residual * residual, axis=1, keepdims=True)
        direction = residual + (power_next / power) * direction
        power = power_next
    return x - damping * delta


def hot_rows(idx_ref):
    rows = [idx_ref[b : b + 1, :] for b in range(idx_ref.shape[0])]
    return [low_hot(row) for row in rows], [high_mask(row) for row in rows]


def first_kernel(x_ref, blk_ref, idx_ref, out_ref):
    hots, masks = hot_rows(idx_ref)
    scattered(x_ref[...], blk_ref, hots, masks, out_ref)


def middle_kernel(x_ref, dual_ref, old_ref, margin_ref, label_ref, blk_ref, idx_ref, x_out, out_ref):
    hots, masks = hot_rows(idx_ref)
    target = old_ref[...] - dual_ref[...]
    x = newton_step(x_ref[...], target, margin_ref[...], label_ref[...], blk_ref, hots, masks)
    x_out[...] = x
    scattered(x, blk_ref, hots, masks, out_ref)


def last_kernel(x_ref, dual_ref, old_ref, margin_ref, label_ref, blk_ref, idx_ref, x_out, sent_ref):
    hots, masks = hot_rows(idx_ref)
    dual = dual_ref[...]
    old = old_ref[...]
    x = newton_step(x_ref[...], old - dual, margin_ref[...], label_ref[...], blk_ref, hots, masks)
    x_out[...] = x
    sent = jnp.concatenate([x, dual, old, jnp.zeros_like(old)], axis=0)
    for peer in range(sent_ref.shape[0]):
        sent_ref[peer] = sent


def full_sum(values):
    return jnp.sum(jnp.sum(values, axis=1, keepdims=True), axis=0, keepdims=True)


def consensus_kernel(came_ref, place_ref, x_ref, dual_ref, cons_ref, dual_out, sums_ref):
    blocks = x_ref.shape[0]
    groups = came_ref.shape[0] // SHARDS
    primal = change = None
    found = []
    for group in range(groups):
        came = [came_ref[group * SHARDS + i] for i in range(SHARDS)]
        solved = [each[:blocks] for each in came]
        old = came[0][2 * blocks : 3 * blocks]
        total = solved[0] + came[0][blocks : 2 * blocks]
        for i in range(1, SHARDS):
            total = total + (solved[i] + came[i][blocks : 2 * blocks])
        averaged = total / float(SHARDS)
        cut = jnp.maximum(jnp.abs(averaged) - threshold, 0.0)
        consensus = jnp.where(averaged < 0.0, -cut, cut)
        found.append(consensus)
        squares = [(each - consensus) ** 2 for each in solved]
        for square in squares:
            primal = square if primal is None else primal + square
        moved = (consensus - old) ** 2
        change = moved if change is None else change + moved
    consensus = found[0]
    for group in range(1, groups):
        own = jnp.broadcast_to(place_ref[:1, :1], consensus.shape) == float(group)
        consensus = jnp.where(own, found[group], consensus)
    cons_ref[...] = consensus
    dual_out[...] = dual_ref[...] + x_ref[...] - consensus
    lane = lax.broadcasted_iota(jnp.int32, (1, LANES), 1)
    sums = jnp.where(
        lane == 0,
        full_sum(primal),
        jnp.where(lane == 1, float(SHARDS) * full_sum(change), 0.0),
    )
    sums_ref[...] = jnp.broadcast_to(sums, sums_ref.shape)


def exchanged(x, axis):
    return lax.all_to_all(x, axis, 0, 0, tiled=True)


def total_of(lines):
    size = lax.axis_size(FEAT)
    parts = exchanged(lines.reshape(size, -1, LANES), FEAT)
    own = jnp.sum(parts, axis=0)
    whole = exchanged(jnp.broadcast_to(own[None], parts.shape), FEAT)
    return whole.reshape(lines.shape)


def local(local_x, dual_var, consensus_old, blocks_data, row_index, labels):
    x = local_x[0]
    dual = dual_var[0]
    blocks = blocks_data[0]
    index = row_index[0]
    marks = labels.reshape(-1, LANES)
    lines = marks.shape
    lanes, size = x.shape
    near = lax.axis_size(NEAR)
    far = lax.axis_size(FAR)
    place = jnp.full((8, LANES), lax.axis_index("feat_2"), jnp.float32)
    (terms,) = call(first_kernel, lines)(x, blocks, index)
    margins = total_of(terms)
    x, terms = call(middle_kernel, x.shape, lines)(
        *in_vmem(x, dual, consensus_old, margins, marks, blocks, index)
    )
    margins = total_of(terms)
    x, sent = call(last_kernel, x.shape, (near, 4 * lanes, size))(
        *in_vmem(x, dual, consensus_old, margins, marks, blocks, index)
    )
    came = exchanged(sent, NEAR)
    consensus, dual_next, sums = call(consensus_kernel, x.shape, x.shape, (far, LANES))(
        *in_vmem(came, place, x, dual)
    )
    sums = jnp.sum(exchanged(sums.reshape(far, 1, LANES), FAR), axis=(0, 1))
    norms = jnp.sqrt(sums[:2]) * jnp.array([1.0, penalty], jnp.float32)
    return (x[None], dual_next[None], consensus, norms)


def solution(mesh):
    if mesh.shape["feat"] == 64:
        feat = (8, 4, 2)
    else:
        feat = (mesh.shape["feat"] // 2, 1, 2)
    torus = Mesh(
        mesh.devices.reshape(*feat, mesh.shape["row"], mesh.shape["col"]), FEAT + SHARD
    )
    placed = (
        P(SHARD, FEAT, None),
        P(SHARD, FEAT, None),
        P(FEAT, None),
        P(SHARD, FEAT, None, None),
        P(SHARD, FEAT, None),
        P(SHARD, None),
    )
    return jax.shard_map(
        local,
        mesh=torus,
        in_specs=placed,
        out_specs=(P(SHARD, FEAT, None), P(SHARD, FEAT, None), P(FEAT, None), P()),
        check_vma=False,
    )
```

```python
import jax
import jax.numpy as jnp
from jax import lax
from jax.experimental import pallas as pl
from jax.experimental.pallas import tpu as pltpu
from jax.sharding import Mesh
from jax.sharding import PartitionSpec as P

CG_STEPS = 3
FEAT = ("feat_0", "feat_1", "feat_2")
SHARD = ("row", "col")
NEAR = ("feat_2", "row", "col")
FAR = ("feat_0", "feat_1")
LANES = 128
HIGH = 64
LOW = 256
SHARDS = 4
INTERPRET = False

penalty = 1.0
damping = 0.5
threshold = 0.05


HBM = pl.BlockSpec(memory_space=pltpu.HBM)


def placed_in(space, args):
    if INTERPRET:
        return args
    return [pltpu.with_memory_space_constraint(arg, space) for arg in args]


def in_vmem(*args):
    return placed_in(pltpu.VMEM, args)


def in_hbm(*args):
    return placed_in(pltpu.HBM, args)


def held(shape, kind=jnp.float32):
    if INTERPRET:
        return jax.ShapeDtypeStruct(shape, kind)
    return pltpu.VMEM(shape, kind)


def call(kernel, *outs, **options):
    return pl.pallas_call(
        kernel,
        out_shape=outs,
        interpret=INTERPRET,
        compiler_params=pltpu.CompilerParams(vmem_limit_bytes=16 << 20),
        **options,
    )


def dot(a, b, dims):
    return lax.dot_general(a, b, (dims, ((), ())), preferred_element_type=jnp.float32)


NN = ((1,), (0,))
NT = ((1,), (1,))


def three_parts(x):
    first = x.astype(jnp.bfloat16).astype(jnp.float32)
    rest = x - first
    second = rest.astype(jnp.bfloat16).astype(jnp.float32)
    return first, second, rest - second


def low_hot(index):
    low = (index & 127) | ((index >> 13) << 7)
    places = lax.broadcasted_iota(jnp.int32, (LOW, index.shape[1]), 0)
    return jnp.where(places == low, 1.0, 0.0).astype(jnp.bfloat16)


def high_mask(index):
    high = (index >> 7) & (HIGH - 1)
    places = lax.broadcasted_iota(jnp.int32, (HIGH, index.shape[1]), 0)
    return places == high


def as_table(lines):
    return jnp.concatenate([lines[:HIGH], lines[HIGH:]], axis=1)


def spread(rounded, turned, hot, mask, b):
    partial = dot(rounded, turned, NN)[b : b + 1]
    parts = [jnp.where(mask, part, 0.0) for part in three_parts(partial)]
    return dot(jnp.concatenate(parts, axis=0).astype(jnp.bfloat16), hot, NT)


def put(table, out_ref):
    table = table[:HIGH] + table[HIGH : 2 * HIGH] + table[2 * HIGH :]
    out_ref[:HIGH, :] = table[:, :LANES]
    out_ref[HIGH:, :] = table[:, LANES:]


def identity_of(size):
    rows = lax.broadcasted_iota(jnp.int32, (size, size), 0)
    cols = lax.broadcasted_iota(jnp.int32, (size, size), 1)
    return jnp.where(rows == cols, 1.0, 0.0)


def newton_step(x, target, margins, labels, blk_ref, turn_ref, hot_ref, masks):
    blocks, size = x.shape
    parts = three_parts(as_table(margins)) + (as_table(labels.astype(jnp.float32)),)
    tables = jnp.concatenate(parts, axis=0).astype(jnp.bfloat16)
    identity = identity_of(size)
    gradients = []
    hessians = []
    for b, mask in enumerate(masks):
        block = blk_ref[b]
        found = dot(tables, hot_ref[b], NN)
        margin = found[:HIGH] + found[HIGH : 2 * HIGH] + found[2 * HIGH : 3 * HIGH]
        margin = jnp.sum(jnp.where(mask, margin, 0.0), axis=0, keepdims=True)
        label = jnp.sum(jnp.where(mask, found[3 * HIGH :], 0.0), axis=0, keepdims=True)
        prob = 1.0 / (1.0 + jnp.exp(-margin))
        misfit = (prob - label).astype(jnp.bfloat16)
        weight = prob * (1.0 - prob)
        gradients.append(dot(misfit, block, NN))
        weighted = (turn_ref[b].astype(jnp.float32) * weight).astype(jnp.bfloat16)
        hessians.append(dot(weighted, block, NN) + penalty * identity)
    gradient = jnp.concatenate(gradients, axis=0) + penalty * (x - target)
    delta = jnp.zeros_like(gradient)
    residual = gradient
    direction = gradient
    power = jnp.sum(residual * residual, axis=1, keepdims=True)
    for cg_step in range(CG_STEPS):
        column = jnp.transpose(jnp.concatenate([direction, direction], axis=0))
        image = jnp.concatenate(
            [
                jnp.sum(hessians[b] * column[:, b : b + 1], axis=0, keepdims=True)
                for b in range(blocks)
            ],
            axis=0,
        )
        alpha = power / jnp.sum(direction * image, axis=1, keepdims=True)
        delta = delta + alpha * direction
        residual = residual - alpha * image
        power_next = jnp.sum(residual * residual, axis=1, keepdims=True)
        direction = residual + (power_next / power) * direction
        power = power_next
    return x - damping * delta


def masks_of(idx_ref):
    return [high_mask(idx_ref[b : b + 1, :]) for b in range(idx_ref.shape[0])]


def first_kernel(place_ref, *refs):
    given, (table_ref, hot_ref, turn_ref, place_out, *kept), (sems, block_sems) = refs[:6], refs[6:-2], refs[-2:]
    (idx_in, x_in, blk_in, *_), (idx_ref, x_ref, blk_ref, *_) = given, kept
    copies = [
        pltpu.make_async_copy(src, dst, sems.at[i])
        for i, (src, dst) in enumerate(zip(given, kept))
        if i != 2
    ]
    blocks = [
        pltpu.make_async_copy(blk_in.at[b], blk_ref.at[b], block_sems.at[b])
        for b in range(blk_ref.shape[0])
    ]
    copies[0].start()
    copies[1].start()
    for copy in blocks:
        copy.start()
    for copy in copies[2:]:
        copy.start()
    place_out[...] = place_ref[...]
    copies[0].wait()
    for b in range(blk_ref.shape[0]):
        hot_ref[b] = low_hot(idx_ref[b : b + 1, :])
    masks = masks_of(idx_ref)
    identity = identity_of(x_ref.shape[1]).astype(jnp.bfloat16)
    copies[1].wait()
    rounded = x_ref[...].astype(jnp.bfloat16)
    table = None
    for b, mask in enumerate(masks):
        blocks[b].wait()
        turned = dot(identity, blk_ref[b], NT).astype(jnp.bfloat16)
        turn_ref[b] = turned
        added = spread(rounded, turned, hot_ref[b], mask, b)
        table = added if table is None else table + added
    put(table, table_ref)
    for copy in copies[2:]:
        copy.wait()


def middle_kernel(margin_ref, hot_ref, turn_ref, idx_ref, x_ref, blk_ref, dual_ref, old_ref, label_ref, x_out, out_ref):
    masks = masks_of(idx_ref)
    target = old_ref[...] - dual_ref[...]
    x = newton_step(
        x_ref[...], target, margin_ref[...], label_ref[...], blk_ref, turn_ref, hot_ref, masks
    )
    x_out[...] = x
    rounded = x.astype(jnp.bfloat16)
    table = None
    for b, mask in enumerate(masks):
        added = spread(rounded, turn_ref[b], hot_ref[b], mask, b)
        table = added if table is None else table + added
    put(table, out_ref)


def last_kernel(
    margin_ref, hot_ref, turn_ref, idx_ref, x_ref, blk_ref, dual_ref, old_ref, label_ref, x_out, sent_ref
):
    masks = masks_of(idx_ref)
    dual = dual_ref[...]
    old = old_ref[...]
    x = newton_step(
        x_ref[...], old - dual, margin_ref[...], label_ref[...], blk_ref, turn_ref, hot_ref, masks
    )
    x_out[...] = x
    sent = jnp.concatenate([x, dual, old, jnp.zeros_like(old)], axis=0)
    for peer in range(sent_ref.shape[0]):
        sent_ref[peer] = sent


def full_sum(values):
    return jnp.sum(jnp.sum(values, axis=1, keepdims=True), axis=0, keepdims=True)


def consensus_kernel(came_ref, place_ref, x_ref, dual_ref, cons_ref, dual_out, sums_ref):
    blocks = x_ref.shape[0]
    groups = came_ref.shape[0] // SHARDS
    primal = change = None
    found = []
    for group in range(groups):
        came = [came_ref[group * SHARDS + i] for i in range(SHARDS)]
        solved = [each[:blocks] for each in came]
        old = came[0][2 * blocks : 3 * blocks]
        total = solved[0] + came[0][blocks : 2 * blocks]
        for i in range(1, SHARDS):
            total = total + (solved[i] + came[i][blocks : 2 * blocks])
        averaged = total / float(SHARDS)
        cut = jnp.maximum(jnp.abs(averaged) - threshold, 0.0)
        consensus = jnp.where(averaged < 0.0, -cut, cut)
        found.append(consensus)
        squares = [(each - consensus) ** 2 for each in solved]
        for square in squares:
            primal = square if primal is None else primal + square
        moved = (consensus - old) ** 2
        change = moved if change is None else change + moved
    consensus = found[0]
    for group in range(1, groups):
        own = jnp.broadcast_to(place_ref[:1, :1], consensus.shape) == float(group)
        consensus = jnp.where(own, found[group], consensus)
    cons_ref[...] = consensus
    dual_out[...] = dual_ref[...] + x_ref[...] - consensus
    lane = lax.broadcasted_iota(jnp.int32, (1, LANES), 1)
    sums = jnp.where(
        lane == 0,
        full_sum(primal),
        jnp.where(lane == 1, float(SHARDS) * full_sum(change), 0.0),
    )
    sums_ref[...] = jnp.broadcast_to(sums, sums_ref.shape)


def finish_kernel(sums_ref, x_ref, dual_ref, cons_ref, x_out, dual_out, cons_out, norms_ref, sems):
    pairs = ((x_ref, x_out), (dual_ref, dual_out), (cons_ref, cons_out))
    copies = [pltpu.make_async_copy(src, dst, sems.at[i]) for i, (src, dst) in enumerate(pairs)]
    for copy in copies:
        copy.start()
    sums = jnp.sqrt(jnp.sum(sums_ref[...], axis=0, keepdims=True))
    lane = lax.broadcasted_iota(jnp.int32, sums.shape, 1)
    norms_ref[0] = jnp.sum(jnp.where(lane == 0, sums, 0.0))
    norms_ref[1] = penalty * jnp.sum(jnp.where(lane == 1, sums, 0.0))
    for copy in copies:
        copy.wait()


def exchanged(x, axis):
    return lax.all_to_all(x, axis, 0, 0, tiled=True)


def total_of(lines):
    size = lax.axis_size(FAR)
    parts = exchanged(lines.reshape(size, -1, LANES), FAR)
    own = jnp.sum(parts, axis=0)
    own = own + lax.ppermute(own, "feat_2", [(0, 1), (1, 0)])
    whole = exchanged(jnp.broadcast_to(own[None], parts.shape), FAR)
    return whole.reshape(lines.shape)


def local(local_x, dual_var, consensus_old, blocks_data, row_index, labels):
    x = local_x[0]
    dual = dual_var[0]
    blocks = blocks_data[0]
    index = row_index[0]
    marks = labels.reshape(-1, LANES)
    lanes, size = x.shape
    rows = index.shape[1]
    near = lax.axis_size(NEAR)
    far = lax.axis_size(FAR)
    place = jnp.full((8, LANES), lax.axis_index("feat_2"), jnp.float32)
    given = (index, x, blocks, dual, consensus_old, marks)
    terms, hots, turned, place, index, x, blocks, dual, old, marks = call(
        first_kernel,
        held(marks.shape),
        held((lanes, LOW, rows), jnp.bfloat16),
        held((lanes, size, rows), jnp.bfloat16),
        held(place.shape),
        *[held(each.shape, each.dtype) for each in given],
        in_specs=[pl.BlockSpec(memory_space=pltpu.VMEM)] + [HBM] * len(given),
        scratch_shapes=[pltpu.SemaphoreType.DMA((len(given),)), pltpu.SemaphoreType.DMA((lanes,))],
    )(*in_vmem(place), *in_hbm(*given))
    kept = (blocks, dual, old, marks)
    margins = total_of(terms)
    x, terms = call(middle_kernel, held(x.shape), held(marks.shape))(
        *in_vmem(margins, hots, turned, index, x, *kept)
    )
    margins = total_of(terms)
    x, sent = call(last_kernel, held(x.shape), held((near, 4 * lanes, size)))(
        *in_vmem(margins, hots, turned, index, x, *kept)
    )
    came = exchanged(sent, NEAR)
    consensus, dual, sums = call(
        consensus_kernel, held(x.shape), held(x.shape), held((far, LANES))
    )(*in_vmem(came, place, x, dual))
    sums = exchanged(sums.reshape(far, 1, LANES), FAR).reshape(far, LANES)
    whole = jax.ShapeDtypeStruct(x.shape, jnp.float32)
    x, dual, consensus, norms = call(
        finish_kernel,
        whole,
        whole,
        whole,
        jax.ShapeDtypeStruct((2,), jnp.float32),
        out_specs=(HBM, HBM, HBM, pl.BlockSpec(memory_space=pltpu.SMEM)),
        scratch_shapes=[pltpu.SemaphoreType.DMA((3,))],
    )(*in_vmem(sums, x, dual, consensus))
    return (x[None], dual[None], consensus, norms)


def solution(mesh):
    if mesh.shape["feat"] == 64:
        feat = (8, 4, 2)
    else:
        feat = (mesh.shape["feat"] // 2, 1, 2)
    torus = Mesh(
        mesh.devices.reshape(*feat, mesh.shape["row"], mesh.shape["col"]), FEAT + SHARD
    )
    placed = (
        P(SHARD, FEAT, None),
        P(SHARD, FEAT, None),
        P(FEAT, None),
        P(SHARD, FEAT, None, None),
        P(SHARD, FEAT, None),
        P(SHARD, None),
    )
    return jax.shard_map(
        local,
        mesh=torus,
        in_specs=placed,
        out_specs=(P(SHARD, FEAT, None), P(SHARD, FEAT, None), P(FEAT, None), P()),
        check_vma=False,
    )
```

```python
import jax
import jax.numpy as jnp
from jax import lax
from jax.experimental import pallas as pl
from jax.experimental.pallas import tpu as pltpu
from jax.sharding import Mesh
from jax.sharding import PartitionSpec as P

CG_STEPS = 3
FEAT = ("feat_0", "feat_1", "feat_2")
SHARD = ("row", "col")
NEAR = ("feat_2", "row", "col")
FAR = ("feat_0", "feat_1")
LANES = 128
HIGH = 64
LOW = 256
SHARDS = 4
INTERPRET = False

penalty = 1.0
damping = 0.5
threshold = 0.05


HBM = pl.BlockSpec(memory_space=pltpu.HBM)


def placed_in(space, args):
    if INTERPRET:
        return args
    return [pltpu.with_memory_space_constraint(arg, space) for arg in args]


def in_vmem(*args):
    return placed_in(pltpu.VMEM, args)


def in_hbm(*args):
    return placed_in(pltpu.HBM, args)


def held(shape, kind=jnp.float32):
    if INTERPRET:
        return jax.ShapeDtypeStruct(shape, kind)
    return pltpu.VMEM(shape, kind)


def call(kernel, *outs, **options):
    return pl.pallas_call(
        kernel,
        out_shape=outs,
        interpret=INTERPRET,
        compiler_params=pltpu.CompilerParams(vmem_limit_bytes=16 << 20),
        **options,
    )


def dot(a, b, dims):
    return lax.dot_general(a, b, (dims, ((), ())), preferred_element_type=jnp.float32)


NN = ((1,), (0,))
NT = ((1,), (1,))


def three_parts(x):
    first = x.astype(jnp.bfloat16).astype(jnp.float32)
    rest = x - first
    second = rest.astype(jnp.bfloat16).astype(jnp.float32)
    return first, second, rest - second


def low_hot(index):
    low = (index & 127) | ((index >> 13) << 7)
    places = lax.broadcasted_iota(jnp.int32, (LOW, index.shape[1]), 0)
    return jnp.where(places == low, 1.0, 0.0).astype(jnp.bfloat16)


def high_mask(index):
    high = (index >> 7) & (HIGH - 1)
    places = lax.broadcasted_iota(jnp.int32, (HIGH, index.shape[1]), 0)
    return places == high


def as_table(lines):
    return jnp.concatenate([lines[:HIGH], lines[HIGH:]], axis=1)


def spread(partial, hot_ref, masks):
    parts = three_parts(partial)
    table = None
    spreads = [
        jnp.concatenate([jnp.where(mask, part[b : b + 1], 0.0) for part in parts], axis=0)
        for b, mask in enumerate(masks)
    ]
    for b, spread_rows in enumerate(spreads):
        added = dot(spread_rows.astype(jnp.bfloat16), hot_ref[b], NT)
        table = added if table is None else table + added
    return table


def put(table, out_ref):
    table = table[:HIGH] + table[HIGH : 2 * HIGH] + table[2 * HIGH :]
    out_ref[:HIGH, :] = table[:, :LANES]
    out_ref[HIGH:, :] = table[:, LANES:]


def identity_of(size):
    rows = lax.broadcasted_iota(jnp.int32, (size, size), 0)
    cols = lax.broadcasted_iota(jnp.int32, (size, size), 1)
    return jnp.where(rows == cols, 1.0, 0.0)


def newton_step(x, target, margins, labels, blk_ref, turn_ref, hot_ref, masks):
    blocks, size = x.shape
    parts = three_parts(as_table(margins)) + (as_table(labels.astype(jnp.float32)),)
    tables = jnp.concatenate(parts, axis=0).astype(jnp.bfloat16)
    found = [dot(tables, hot_ref[b], NN) for b in range(blocks)]
    margin = []
    label = []
    for each, mask in zip(found, masks):
        whole = each[:HIGH] + each[HIGH : 2 * HIGH] + each[2 * HIGH : 3 * HIGH]
        margin.append(jnp.sum(jnp.where(mask, whole, 0.0), axis=0, keepdims=True))
        label.append(jnp.sum(jnp.where(mask, each[3 * HIGH :], 0.0), axis=0, keepdims=True))
    prob = 1.0 / (1.0 + jnp.exp(-jnp.concatenate(margin, axis=0)))
    misfit = (prob - jnp.concatenate(label, axis=0)).astype(jnp.bfloat16)
    weight = prob * (1.0 - prob)
    identity = penalty * identity_of(size)
    gradients = [dot(misfit, blk_ref[b], NN)[b : b + 1] for b in range(blocks)]
    weighted = [
        (turn_ref[b].astype(jnp.float32) * weight[b : b + 1]).astype(jnp.bfloat16)
        for b in range(blocks)
    ]
    hessians = [dot(weighted[b], blk_ref[b], NN) + identity for b in range(blocks)]
    gradient = jnp.concatenate(gradients, axis=0) + penalty * (x - target)
    delta = jnp.zeros_like(gradient)
    residual = gradient
    direction = gradient
    power = jnp.sum(residual * residual, axis=1, keepdims=True)
    for cg_step in range(CG_STEPS):
        column = jnp.transpose(jnp.concatenate([direction, direction], axis=0))
        image = jnp.concatenate(
            [
                jnp.sum(hessians[b] * column[:, b : b + 1], axis=0, keepdims=True)
                for b in range(blocks)
            ],
            axis=0,
        )
        alpha = power / jnp.sum(direction * image, axis=1, keepdims=True)
        delta = delta + alpha * direction
        residual = residual - alpha * image
        power_next = jnp.sum(residual * residual, axis=1, keepdims=True)
        direction = residual + (power_next / power) * direction
        power = power_next
    return x - damping * delta


def masks_of(idx_ref):
    return [high_mask(idx_ref[b : b + 1, :]) for b in range(idx_ref.shape[0])]


def first_kernel(place_ref, *refs):
    given, (table_ref, hot_ref, turn_ref, place_out, *kept), (sems, block_sems) = refs[:6], refs[6:-2], refs[-2:]
    (idx_in, x_in, blk_in, *_), (idx_ref, x_ref, blk_ref, *_) = given, kept
    copies = [
        pltpu.make_async_copy(src, dst, sems.at[i])
        for i, (src, dst) in enumerate(zip(given, kept))
        if i != 2
    ]
    blocks = [
        pltpu.make_async_copy(blk_in.at[b], blk_ref.at[b], block_sems.at[b])
        for b in range(blk_ref.shape[0])
    ]
    copies[0].start()
    copies[1].start()
    for copy in blocks:
        copy.start()
    for copy in copies[2:]:
        copy.start()
    place_out[...] = place_ref[...]
    copies[0].wait()
    for b in range(blk_ref.shape[0]):
        hot_ref[b] = low_hot(idx_ref[b : b + 1, :])
    masks = masks_of(idx_ref)
    copies[1].wait()
    x = x_ref[...]
    left = jnp.concatenate([identity_of(x.shape[1])] + [x] * (16 // x.shape[0]), axis=0)
    left = left.astype(jnp.bfloat16)
    for copy in blocks:
        copy.wait()
    partial = []
    for b in range(blk_ref.shape[0]):
        both = dot(left, blk_ref[b], NT)
        turn_ref[b] = both[: x.shape[1]].astype(jnp.bfloat16)
        partial.append(both[x.shape[1] + b : x.shape[1] + b + 1])
    put(spread(jnp.concatenate(partial, axis=0), hot_ref, masks), table_ref)
    for copy in copies[2:]:
        copy.wait()


def summed(margin_ref):
    lines = LANES
    total = margin_ref[:lines]
    for start in range(lines, margin_ref.shape[0], lines):
        total = total + margin_ref[start : start + lines]
    return total


def middle_kernel(margin_ref, hot_ref, turn_ref, idx_ref, x_ref, blk_ref, dual_ref, old_ref, label_ref, x_out, out_ref):
    masks = masks_of(idx_ref)
    target = old_ref[...] - dual_ref[...]
    x = newton_step(
        x_ref[...], target, summed(margin_ref), label_ref[...], blk_ref, turn_ref, hot_ref, masks
    )
    x_out[...] = x
    rounded = x.astype(jnp.bfloat16)
    partial = [dot(rounded, turn_ref[b], NN)[b : b + 1] for b in range(x.shape[0])]
    put(spread(jnp.concatenate(partial, axis=0), hot_ref, masks), out_ref)


def last_kernel(
    margin_ref, hot_ref, turn_ref, idx_ref, x_ref, blk_ref, dual_ref, old_ref, label_ref, x_out, sent_ref
):
    masks = masks_of(idx_ref)
    dual = dual_ref[...]
    old = old_ref[...]
    x = newton_step(
        x_ref[...], old - dual, summed(margin_ref), label_ref[...], blk_ref, turn_ref, hot_ref, masks
    )
    x_out[...] = x
    sent = jnp.concatenate([x, dual, old, jnp.zeros_like(old)], axis=0)
    for peer in range(sent_ref.shape[0]):
        sent_ref[peer] = sent


def full_sum(values):
    return jnp.sum(jnp.sum(values, axis=1, keepdims=True), axis=0, keepdims=True)


def consensus_kernel(came_ref, place_ref, x_ref, dual_ref, cons_ref, dual_out, sums_ref):
    blocks = x_ref.shape[0]
    groups = came_ref.shape[0] // SHARDS
    primal = change = None
    found = []
    for group in range(groups):
        came = [came_ref[group * SHARDS + i] for i in range(SHARDS)]
        solved = [each[:blocks] for each in came]
        old = came[0][2 * blocks : 3 * blocks]
        total = solved[0] + came[0][blocks : 2 * blocks]
        for i in range(1, SHARDS):
            total = total + (solved[i] + came[i][blocks : 2 * blocks])
        averaged = total / float(SHARDS)
        cut = jnp.maximum(jnp.abs(averaged) - threshold, 0.0)
        consensus = jnp.where(averaged < 0.0, -cut, cut)
        found.append(consensus)
        squares = [(each - consensus) ** 2 for each in solved]
        for square in squares:
            primal = square if primal is None else primal + square
        moved = (consensus - old) ** 2
        change = moved if change is None else change + moved
    consensus = found[0]
    for group in range(1, groups):
        own = jnp.broadcast_to(place_ref[:1, :1], consensus.shape) == float(group)
        consensus = jnp.where(own, found[group], consensus)
    cons_ref[...] = consensus
    dual_out[...] = dual_ref[...] + x_ref[...] - consensus
    lane = lax.broadcasted_iota(jnp.int32, (1, LANES), 1)
    sums = jnp.where(
        lane == 0,
        full_sum(primal),
        jnp.where(lane == 1, float(SHARDS) * full_sum(change), 0.0),
    )
    sums_ref[...] = jnp.broadcast_to(sums, sums_ref.shape)


def finish_kernel(sums_ref, x_ref, dual_ref, cons_ref, x_out, dual_out, cons_out, norms_out, norms_ref, sems):
    pairs = ((x_ref, x_out), (dual_ref, dual_out), (cons_ref, cons_out))
    copies = [pltpu.make_async_copy(src, dst, sems.at[i]) for i, (src, dst) in enumerate(pairs)]
    for copy in copies:
        copy.start()
    sums = jnp.sqrt(jnp.sum(sums_ref[...], axis=0, keepdims=True))
    lane = lax.broadcasted_iota(jnp.int32, sums.shape, 1)
    norms_ref[...] = jnp.where(lane == 1, penalty * sums, sums)[0, :2]
    last = pltpu.make_async_copy(norms_ref, norms_out, sems.at[len(copies)])
    last.start()
    for copy in copies + [last]:
        copy.wait()


def exchanged(x, axis):
    return lax.all_to_all(x, axis, 0, 0, tiled=True)


def tables_to_sum(lines):
    far = lax.axis_size(FAR)
    parts = exchanged(lines.reshape(far, -1, LANES), FAR)
    own = jnp.sum(parts, axis=0)
    copies = jnp.broadcast_to(own[None], (lax.axis_size("feat_2") * far, *own.shape))
    return exchanged(copies, ("feat_2",) + FAR).reshape(-1, LANES)


def local(local_x, dual_var, consensus_old, blocks_data, row_index, labels):
    x = local_x[0]
    dual = dual_var[0]
    blocks = blocks_data[0]
    index = row_index[0]
    marks = labels.reshape(-1, LANES)
    lanes, size = x.shape
    rows = index.shape[1]
    near = lax.axis_size(NEAR)
    far = lax.axis_size(FAR)
    place = jnp.full((8, LANES), lax.axis_index("feat_2"), jnp.float32)
    given = (index, x, blocks, dual, consensus_old, marks)
    terms, hots, turned, place, index, x, blocks, dual, old, marks = call(
        first_kernel,
        held(marks.shape),
        held((lanes, LOW, rows), jnp.bfloat16),
        held((lanes, size, rows), jnp.bfloat16),
        held(place.shape),
        *[held(each.shape, each.dtype) for each in given],
        in_specs=[pl.BlockSpec(memory_space=pltpu.VMEM)] + [HBM] * len(given),
        scratch_shapes=[pltpu.SemaphoreType.DMA((len(given),)), pltpu.SemaphoreType.DMA((lanes,))],
    )(*in_vmem(place), *in_hbm(*given))
    kept = (blocks, dual, old, marks)
    margins = tables_to_sum(terms)
    x, terms = call(middle_kernel, held(x.shape), held(marks.shape))(
        *in_vmem(margins, hots, turned, index, x, *kept)
    )
    margins = tables_to_sum(terms)
    x, sent = call(last_kernel, held(x.shape), held((near, 4 * lanes, size)))(
        *in_vmem(margins, hots, turned, index, x, *kept)
    )
    came = exchanged(sent, NEAR)
    consensus, dual, sums = call(
        consensus_kernel, held(x.shape), held(x.shape), held((far, LANES))
    )(*in_vmem(came, place, x, dual))
    sums = exchanged(sums.reshape(far, 1, LANES), FAR).reshape(far, LANES)
    whole = jax.ShapeDtypeStruct(x.shape, jnp.float32)
    x, dual, consensus, norms = call(
        finish_kernel,
        whole,
        whole,
        whole,
        jax.ShapeDtypeStruct((2,), jnp.float32),
        out_specs=(HBM, HBM, HBM, HBM),
        scratch_shapes=[pltpu.VMEM((2,), jnp.float32), pltpu.SemaphoreType.DMA((4,))],
    )(*in_vmem(sums, x, dual, consensus))
    return (x[None], dual[None], consensus, norms)


def solution(mesh):
    if mesh.shape["feat"] == 64:
        feat = (8, 4, 2)
    else:
        feat = (mesh.shape["feat"] // 2, 1, 2)
    torus = Mesh(
        mesh.devices.reshape(*feat, mesh.shape["row"], mesh.shape["col"]), FEAT + SHARD
    )
    placed = (
        P(SHARD, FEAT, None),
        P(SHARD, FEAT, None),
        P(FEAT, None),
        P(SHARD, FEAT, None, None),
        P(SHARD, FEAT, None),
        P(SHARD, None),
    )
    return jax.shard_map(
        local,
        mesh=torus,
        in_specs=placed,
        out_specs=(P(SHARD, FEAT, None), P(SHARD, FEAT, None), P(FEAT, None), P()),
        check_vma=False,
    )
```

```python
import jax
import jax.numpy as jnp
from jax import lax
from jax.experimental import pallas as pl
from jax.experimental.pallas import tpu as pltpu
from jax.sharding import Mesh
from jax.sharding import PartitionSpec as P

CG_STEPS = 3
FEAT = ("feat_0", "feat_1", "feat_2")
SHARD = ("row", "col")
NEAR = ("feat_2", "row", "col")
FAR = ("feat_0", "feat_1")
LANES = 128
HIGH = 64
LOW = 256
SHARDS = 4
INTERPRET = False

penalty = 1.0
damping = 0.5
threshold = 0.05


HBM = pl.BlockSpec(memory_space=pltpu.HBM)


def placed_in(space, args):
    if INTERPRET:
        return args
    return [pltpu.with_memory_space_constraint(arg, space) for arg in args]


def in_vmem(*args):
    return placed_in(pltpu.VMEM, args)


def in_hbm(*args):
    return placed_in(pltpu.HBM, args)


def held(shape, kind=jnp.float32):
    if INTERPRET:
        return jax.ShapeDtypeStruct(shape, kind)
    return pltpu.VMEM(shape, kind)


def call(kernel, *outs, **options):
    return pl.pallas_call(
        kernel,
        out_shape=outs,
        interpret=INTERPRET,
        compiler_params=pltpu.CompilerParams(vmem_limit_bytes=16 << 20),
        **options,
    )


def dot(a, b, dims):
    return lax.dot_general(a, b, (dims, ((), ())), preferred_element_type=jnp.float32)


NN = ((1,), (0,))
NT = ((1,), (1,))


def three_parts(x):
    first = x.astype(jnp.bfloat16).astype(jnp.float32)
    rest = x - first
    second = rest.astype(jnp.bfloat16).astype(jnp.float32)
    return first, second, rest - second


def low_hot(index):
    low = (index & 127) | ((index >> 13) << 7)
    places = lax.broadcasted_iota(jnp.int32, (LOW, index.shape[1]), 0)
    return jnp.where(places == low, 1.0, 0.0).astype(jnp.bfloat16)


def high_mask(index):
    high = (index >> 7) & (HIGH - 1)
    places = lax.broadcasted_iota(jnp.int32, (HIGH, index.shape[1]), 0)
    return places == high


def as_table(lines):
    return jnp.concatenate([lines[:HIGH], lines[HIGH:]], axis=1)


def spread(partial, hot_ref, masks):
    parts = three_parts(partial)
    table = None
    spreads = [
        jnp.concatenate([jnp.where(mask, part[b : b + 1], 0.0) for part in parts], axis=0)
        for b, mask in enumerate(masks)
    ]
    for b, spread_rows in enumerate(spreads):
        added = dot(spread_rows.astype(jnp.bfloat16), hot_ref[b], NT)
        table = added if table is None else table + added
    return table


def put(table, out_ref):
    table = table[:HIGH] + table[HIGH : 2 * HIGH] + table[2 * HIGH :]
    out_ref[:HIGH, :] = table[:, :LANES]
    out_ref[HIGH:, :] = table[:, LANES:]


def picked(found, masks):
    rows = [
        jnp.sum(jnp.where(mask, each, 0.0), axis=0, keepdims=True)
        for each, mask in zip(found, masks)
    ]
    return jnp.concatenate(rows, axis=0)


def identity_of(size):
    rows = lax.broadcasted_iota(jnp.int32, (size, size), 0)
    cols = lax.broadcasted_iota(jnp.int32, (size, size), 1)
    return jnp.where(rows == cols, 1.0, 0.0)


def as_column(line):
    size = line.shape[1]
    pieces = [
        jnp.transpose(jnp.broadcast_to(line[:, start : start + LANES], (LANES, LANES)))
        for start in range(0, size, LANES)
    ]
    return jnp.concatenate([jnp.concatenate(pieces, axis=0)] * (size // LANES), axis=1)


def newton_step(x, target, margins, labels, blk_ref, turn_ref, hot_ref, masks):
    blocks, size = x.shape
    tables = jnp.concatenate(three_parts(as_table(margins)), axis=0).astype(jnp.bfloat16)
    found = [dot(tables, hot_ref[b], NN) for b in range(blocks)]
    found = [each[:HIGH] + each[HIGH : 2 * HIGH] + each[2 * HIGH :] for each in found]
    prob = 1.0 / (1.0 + jnp.exp(-picked(found, masks)))
    misfit = (prob - labels).astype(jnp.bfloat16)
    weight = prob * (1.0 - prob)
    identity = penalty * identity_of(size)
    gradients = [dot(misfit, blk_ref[b], NN)[b : b + 1] for b in range(blocks)]
    weighted = [
        (turn_ref[b].astype(jnp.float32) * weight[b : b + 1]).astype(jnp.bfloat16)
        for b in range(blocks)
    ]
    hessians = [dot(weighted[b], blk_ref[b], NN) + identity for b in range(blocks)]
    gradient = jnp.concatenate(gradients, axis=0) + penalty * (x - target)
    delta = jnp.zeros_like(gradient)
    residual = gradient
    direction = gradient
    power = jnp.sum(residual * residual, axis=1, keepdims=True)
    for cg_step in range(CG_STEPS):
        image = jnp.concatenate(
            [
                jnp.sum(hessians[b] * as_column(direction[b : b + 1]), axis=0, keepdims=True)
                for b in range(blocks)
            ],
            axis=0,
        )
        alpha = power / jnp.sum(direction * image, axis=1, keepdims=True)
        delta = delta + alpha * direction
        residual = residual - alpha * image
        power_next = jnp.sum(residual * residual, axis=1, keepdims=True)
        direction = residual + (power_next / power) * direction
        power = power_next
    return x - damping * delta


def masks_of(idx_ref):
    return [high_mask(idx_ref[b : b + 1, :]) for b in range(idx_ref.shape[0])]


def first_kernel(place_ref, *refs):
    given, (table_ref, hot_ref, turn_ref, place_out, label_ref, *kept), scratch = refs[:6], refs[6:-3], refs[-3:]
    marks_ref, sems, block_sems = scratch
    kept = (*kept, marks_ref)
    (idx_in, x_in, blk_in, *_), (idx_ref, x_ref, blk_ref, *_) = given, kept
    copies = [
        pltpu.make_async_copy(src, dst, sems.at[i])
        for i, (src, dst) in enumerate(zip(given, kept))
        if i != 2
    ]
    blocks = [
        pltpu.make_async_copy(blk_in.at[b], blk_ref.at[b], block_sems.at[b])
        for b in range(blk_ref.shape[0])
    ]
    for copy in (copies[0], copies[1], copies[-1], *blocks, *copies[2:-1]):
        copy.start()
    place_out[...] = place_ref[...]
    copies[0].wait()
    for b in range(blk_ref.shape[0]):
        hot_ref[b] = low_hot(idx_ref[b : b + 1, :])
    masks = masks_of(idx_ref)
    copies[-1].wait()
    marks = as_table(marks_ref[...].astype(jnp.float32)).astype(jnp.bfloat16)
    found = [dot(marks, hot_ref[b], NN) for b in range(blk_ref.shape[0])]
    label_ref[...] = picked(found, masks)
    copies[1].wait()
    x = x_ref[...]
    left = jnp.concatenate([identity_of(x.shape[1])] + [x] * (16 // x.shape[0]), axis=0)
    left = left.astype(jnp.bfloat16)
    for copy in blocks:
        copy.wait()
    partial = []
    for b in range(blk_ref.shape[0]):
        both = dot(left, blk_ref[b], NT)
        turn_ref[b] = both[: x.shape[1]].astype(jnp.bfloat16)
        partial.append(both[x.shape[1] + b : x.shape[1] + b + 1])
    put(spread(jnp.concatenate(partial, axis=0), hot_ref, masks), table_ref)
    for copy in copies[2:-1]:
        copy.wait()


def summed(margin_ref):
    lines = LANES
    total = margin_ref[:lines]
    for start in range(lines, margin_ref.shape[0], lines):
        total = total + margin_ref[start : start + lines]
    return total


def middle_kernel(margin_ref, hot_ref, turn_ref, idx_ref, x_ref, blk_ref, dual_ref, old_ref, label_ref, x_out, out_ref):
    masks = masks_of(idx_ref)
    target = old_ref[...] - dual_ref[...]
    x = newton_step(
        x_ref[...], target, summed(margin_ref), label_ref[...], blk_ref, turn_ref, hot_ref, masks
    )
    x_out[...] = x
    rounded = x.astype(jnp.bfloat16)
    partial = [dot(rounded, turn_ref[b], NN)[b : b + 1] for b in range(x.shape[0])]
    put(spread(jnp.concatenate(partial, axis=0), hot_ref, masks), out_ref)


def last_kernel(
    margin_ref, hot_ref, turn_ref, idx_ref, x_ref, blk_ref, dual_ref, old_ref, label_ref, x_out, sent_ref
):
    masks = masks_of(idx_ref)
    dual = dual_ref[...]
    old = old_ref[...]
    x = newton_step(
        x_ref[...], old - dual, summed(margin_ref), label_ref[...], blk_ref, turn_ref, hot_ref, masks
    )
    x_out[...] = x
    for peer in range(sent_ref.shape[0]):
        for i, sent in enumerate((x, dual, old)):
            sent_ref[peer, i] = sent


def full_sum(values):
    return jnp.sum(jnp.sum(values, axis=1, keepdims=True), axis=0, keepdims=True)


def consensus_kernel(came_ref, place_ref, x_ref, dual_ref, cons_ref, dual_out, sums_ref):
    groups = came_ref.shape[0] // SHARDS
    primal = change = None
    found = []
    for group in range(groups):
        peers = range(group * SHARDS, (group + 1) * SHARDS)
        solved = [came_ref[i, 0] for i in peers]
        both = [came_ref[i, 0] + came_ref[i, 1] for i in peers]
        old = came_ref[group * SHARDS, 2]
        total = both[0]
        for each in both[1:]:
            total = total + each
        averaged = total / float(SHARDS)
        cut = jnp.maximum(jnp.abs(averaged) - threshold, 0.0)
        consensus = jnp.where(averaged < 0.0, -cut, cut)
        found.append(consensus)
        squares = [(each - consensus) ** 2 for each in solved]
        for square in squares:
            primal = square if primal is None else primal + square
        moved = (consensus - old) ** 2
        change = moved if change is None else change + moved
    consensus = found[0]
    for group in range(1, groups):
        own = jnp.broadcast_to(place_ref[:1, :1], consensus.shape) == float(group)
        consensus = jnp.where(own, found[group], consensus)
    cons_ref[...] = consensus
    dual_out[...] = dual_ref[...] + x_ref[...] - consensus
    lane = lax.broadcasted_iota(jnp.int32, (1, LANES), 1)
    sums = jnp.where(
        lane == 0,
        full_sum(primal),
        jnp.where(lane == 1, float(SHARDS) * full_sum(change), 0.0),
    )
    sums_ref[...] = jnp.broadcast_to(sums, sums_ref.shape)


def finish_kernel(sums_ref, x_ref, dual_ref, cons_ref, x_out, dual_out, cons_out, norms_out, norms_ref, sems):
    pairs = ((x_ref, x_out), (dual_ref, dual_out), (cons_ref, cons_out))
    copies = [pltpu.make_async_copy(src, dst, sems.at[i]) for i, (src, dst) in enumerate(pairs)]
    for copy in copies:
        copy.start()
    sums = jnp.sqrt(jnp.sum(sums_ref[...], axis=0, keepdims=True))
    lane = lax.broadcasted_iota(jnp.int32, sums.shape, 1)
    norms_ref[...] = jnp.where(lane == 1, penalty * sums, sums)[0, :2]
    last = pltpu.make_async_copy(norms_ref, norms_out, sems.at[len(copies)])
    last.start()
    for copy in copies + [last]:
        copy.wait()


def exchanged(x, axis):
    return lax.all_to_all(x, axis, 0, 0, tiled=True)


def tables_to_sum(lines):
    far = lax.axis_size(FAR)
    parts = exchanged(lines.reshape(far, -1, LANES), FAR)
    own = jnp.sum(parts, axis=0)
    copies = jnp.broadcast_to(own[None], (lax.axis_size("feat_2") * far, *own.shape))
    return exchanged(copies, ("feat_2",) + FAR).reshape(-1, LANES)


def local(local_x, dual_var, consensus_old, blocks_data, row_index, labels):
    x = local_x[0]
    dual = dual_var[0]
    blocks = blocks_data[0]
    index = row_index[0]
    marks = labels.reshape(-1, LANES)
    lanes, size = x.shape
    rows = index.shape[1]
    near = lax.axis_size(NEAR)
    far = lax.axis_size(FAR)
    place = jnp.full((8, LANES), lax.axis_index("feat_2"), jnp.float32)
    given = (index, x, blocks, dual, consensus_old, marks)
    terms, hots, turned, place, label, index, x, blocks, dual, old = call(
        first_kernel,
        held(marks.shape),
        held((lanes, LOW, rows), jnp.bfloat16),
        held((lanes, size, rows), jnp.bfloat16),
        held(place.shape),
        held(index.shape),
        *[held(each.shape, each.dtype) for each in given[:-1]],
        in_specs=[pl.BlockSpec(memory_space=pltpu.VMEM)] + [HBM] * len(given),
        scratch_shapes=[
            pltpu.VMEM(marks.shape, marks.dtype),
            pltpu.SemaphoreType.DMA((len(given),)),
            pltpu.SemaphoreType.DMA((lanes,)),
        ],
    )(*in_vmem(place), *in_hbm(*given))
    kept = (blocks, dual, old, label)
    margins = tables_to_sum(terms)
    x, terms = call(middle_kernel, held(x.shape), held(marks.shape))(
        *in_vmem(margins, hots, turned, index, x, *kept)
    )
    margins = tables_to_sum(terms)
    x, sent = call(last_kernel, held(x.shape), held((near, 3, lanes, size)))(
        *in_vmem(margins, hots, turned, index, x, *kept)
    )
    came = exchanged(sent, NEAR)
    consensus, dual, sums = call(
        consensus_kernel, held(x.shape), held(x.shape), held((far, LANES))
    )(*in_vmem(came, place, x, dual))
    sums = exchanged(sums.reshape(far, 1, LANES), FAR).reshape(far, LANES)
    whole = jax.ShapeDtypeStruct(x.shape, jnp.float32)
    x, dual, consensus, norms = call(
        finish_kernel,
        whole,
        whole,
        whole,
        jax.ShapeDtypeStruct((2,), jnp.float32),
        out_specs=(HBM, HBM, HBM, HBM),
        scratch_shapes=[pltpu.VMEM((2,), jnp.float32), pltpu.SemaphoreType.DMA((4,))],
    )(*in_vmem(sums, x, dual, consensus))
    return (x[None], dual[None], consensus, norms)


def solution(mesh):
    if mesh.shape["feat"] == 64:
        feat = (8, 4, 2)
    else:
        feat = (mesh.shape["feat"] // 2, 1, 2)
    torus = Mesh(
        mesh.devices.reshape(*feat, mesh.shape["row"], mesh.shape["col"]), FEAT + SHARD
    )
    placed = (
        P(SHARD, FEAT, None),
        P(SHARD, FEAT, None),
        P(FEAT, None),
        P(SHARD, FEAT, None, None),
        P(SHARD, FEAT, None),
        P(SHARD, None),
    )
    return jax.shard_map(
        local,
        mesh=torus,
        in_specs=placed,
        out_specs=(P(SHARD, FEAT, None), P(SHARD, FEAT, None), P(FEAT, None), P()),
        check_vma=False,
    )
```

```python
import jax
import jax.numpy as jnp
from jax import lax
from jax.experimental import pallas as pl
from jax.experimental.pallas import tpu as pltpu
from jax.sharding import Mesh
from jax.sharding import PartitionSpec as P

CG_STEPS = 3
FEAT = ("feat_0", "feat_1", "feat_2")
SHARD = ("row", "col")
NEAR = ("feat_2", "row", "col")
FAR = ("feat_0", "feat_1")
LANES = 128
HIGH = 64
LOW = 256
SHARDS = 4
INTERPRET = False

penalty = 1.0
damping = 0.5
threshold = 0.05


HBM = pl.BlockSpec(memory_space=pltpu.HBM)


def placed_in(space, args):
    if INTERPRET:
        return args
    return [pltpu.with_memory_space_constraint(arg, space) for arg in args]


def in_vmem(*args):
    return placed_in(pltpu.VMEM, args)


def in_hbm(*args):
    return placed_in(pltpu.HBM, args)


def held(shape, kind=jnp.float32):
    if INTERPRET:
        return jax.ShapeDtypeStruct(shape, kind)
    return pltpu.VMEM(shape, kind)


def call(kernel, *outs, **options):
    return pl.pallas_call(
        kernel,
        out_shape=outs,
        interpret=INTERPRET,
        compiler_params=pltpu.CompilerParams(vmem_limit_bytes=16 << 20),
        **options,
    )


def dot(a, b, dims):
    return lax.dot_general(a, b, (dims, ((), ())), preferred_element_type=jnp.float32)


NN = ((1,), (0,))
NT = ((1,), (1,))


def three_parts(x):
    first = x.astype(jnp.bfloat16).astype(jnp.float32)
    rest = x - first
    second = rest.astype(jnp.bfloat16).astype(jnp.float32)
    return first, second, rest - second


def low_hot(index):
    low = (index & 127) | ((index >> 13) << 7)
    places = lax.broadcasted_iota(jnp.int32, (LOW, index.shape[1]), 0)
    return jnp.where(places == low, 1.0, 0.0).astype(jnp.bfloat16)


def high_mask(index):
    high = (index >> 7) & (HIGH - 1)
    places = lax.broadcasted_iota(jnp.int32, (HIGH, index.shape[1]), 0)
    return places == high


def as_table(lines):
    return jnp.concatenate([lines[:HIGH], lines[HIGH:]], axis=1)


def spread(partial, hot_ref, masks, dims):
    parts = three_parts(partial)
    table = None
    spreads = [
        jnp.concatenate([jnp.where(mask, part[b : b + 1], 0.0) for part in parts], axis=0)
        for b, mask in enumerate(masks)
    ]
    for b, spread_rows in enumerate(spreads):
        added = dot(spread_rows.astype(jnp.bfloat16), hot_ref[b], dims)
        table = added if table is None else table + added
    return table


def put(table, out_ref):
    table = table[:HIGH] + table[HIGH : 2 * HIGH] + table[2 * HIGH :]
    out_ref[:HIGH, :] = table[:, :LANES]
    out_ref[HIGH:, :] = table[:, LANES:]


def picked(found, masks):
    rows = [
        jnp.sum(jnp.where(mask, each, 0.0), axis=0, keepdims=True)
        for each, mask in zip(found, masks)
    ]
    return jnp.concatenate(rows, axis=0)


def identity_of(size):
    rows = lax.broadcasted_iota(jnp.int32, (size, size), 0)
    cols = lax.broadcasted_iota(jnp.int32, (size, size), 1)
    return jnp.where(rows == cols, 1.0, 0.0)


def as_column(line):
    size = line.shape[1]
    pieces = [
        jnp.transpose(jnp.broadcast_to(line[:, start : start + LANES], (LANES, LANES)))
        for start in range(0, size, LANES)
    ]
    return jnp.concatenate([jnp.concatenate(pieces, axis=0)] * (size // LANES), axis=1)


def newton_step(x, target, margins, labels, blk_ref, turn_ref, hot_ref, masks):
    blocks, size = x.shape
    tables = jnp.concatenate(three_parts(as_table(margins)), axis=0).astype(jnp.bfloat16)
    found = [dot(tables, hot_ref[b], NN) for b in range(blocks)]
    found = [each[:HIGH] + each[HIGH : 2 * HIGH] + each[2 * HIGH :] for each in found]
    prob = 1.0 / (1.0 + jnp.exp(-picked(found, masks)))
    misfit = (prob - labels).astype(jnp.bfloat16)
    weight = prob * (1.0 - prob)
    identity = penalty * identity_of(size)
    gradients = [dot(misfit, blk_ref[b], NN)[b : b + 1] for b in range(blocks)]
    weighted = [
        (turn_ref[b].astype(jnp.float32) * weight[b : b + 1]).astype(jnp.bfloat16)
        for b in range(blocks)
    ]
    hessians = [dot(weighted[b], blk_ref[b], NN) + identity for b in range(blocks)]
    gradient = jnp.concatenate(gradients, axis=0) + penalty * (x - target)
    delta = jnp.zeros_like(gradient)
    residual = gradient
    direction = gradient
    power = jnp.sum(residual * residual, axis=1, keepdims=True)
    for cg_step in range(CG_STEPS):
        image = jnp.concatenate(
            [
                jnp.sum(hessians[b] * as_column(direction[b : b + 1]), axis=0, keepdims=True)
                for b in range(blocks)
            ],
            axis=0,
        )
        alpha = power / jnp.sum(direction * image, axis=1, keepdims=True)
        delta = delta + alpha * direction
        residual = residual - alpha * image
        power_next = jnp.sum(residual * residual, axis=1, keepdims=True)
        direction = residual + (power_next / power) * direction
        power = power_next
    return x - damping * delta


def masks_of(idx_ref):
    return [high_mask(idx_ref[b : b + 1, :]) for b in range(idx_ref.shape[0])]


def first_kernel(place_ref, *refs):
    given, (table_ref, hot_ref, turn_ref, place_out, label_ref, *kept), scratch = refs[:6], refs[6:-3], refs[-3:]
    marks_ref, sems, block_sems = scratch
    kept = (*kept, marks_ref)
    (idx_in, x_in, blk_in, *_), (idx_ref, x_ref, blk_ref, *_) = given, kept
    copies = [
        pltpu.make_async_copy(src, dst, sems.at[i])
        for i, (src, dst) in enumerate(zip(given, kept))
        if i != 2
    ]
    blocks = [
        pltpu.make_async_copy(blk_in.at[b], blk_ref.at[b], block_sems.at[b])
        for b in range(blk_ref.shape[0])
    ]
    for copy in (copies[0], copies[1], copies[-1], *blocks, *copies[2:-1]):
        copy.start()
    place_out[...] = place_ref[...]
    copies[0].wait()
    for b in range(blk_ref.shape[0]):
        hot_ref[b] = low_hot(idx_ref[b : b + 1, :])
    masks = masks_of(idx_ref)
    copies[-1].wait()
    marks = as_table(marks_ref[...].astype(jnp.float32)).astype(jnp.bfloat16)
    found = [dot(marks, hot_ref[b], NN) for b in range(blk_ref.shape[0])]
    label_ref[...] = picked(found, masks)
    copies[1].wait()
    rounded = x_ref[...].astype(jnp.bfloat16)
    for copy in blocks:
        copy.wait()
    partial = []
    for b in range(blk_ref.shape[0]):
        turned = jnp.transpose(blk_ref[b])
        turn_ref[b] = turned
        partial.append(dot(rounded, turned, NN)[b : b + 1])
    put(spread(jnp.concatenate(partial, axis=0), hot_ref, masks, NT), table_ref)
    for copy in copies[2:-1]:
        copy.wait()


def summed(margin_ref):
    lines = LANES
    total = margin_ref[:lines]
    for start in range(lines, margin_ref.shape[0], lines):
        total = total + margin_ref[start : start + lines]
    return total


def middle_kernel(margin_ref, hot_ref, turn_ref, idx_ref, x_ref, blk_ref, dual_ref, old_ref, label_ref, x_out, out_ref, stood_ref):
    masks = masks_of(idx_ref)
    for b in range(x_ref.shape[0]):
        stood_ref[b] = jnp.transpose(hot_ref[b])
    target = old_ref[...] - dual_ref[...]
    x = newton_step(
        x_ref[...], target, summed(margin_ref), label_ref[...], blk_ref, turn_ref, hot_ref, masks
    )
    x_out[...] = x
    rounded = x.astype(jnp.bfloat16)
    partial = [dot(rounded, turn_ref[b], NN)[b : b + 1] for b in range(x.shape[0])]
    put(spread(jnp.concatenate(partial, axis=0), stood_ref, masks, NN), out_ref)


def last_kernel(
    margin_ref, hot_ref, turn_ref, idx_ref, x_ref, blk_ref, dual_ref, old_ref, label_ref, x_out, sent_ref
):
    masks = masks_of(idx_ref)
    dual = dual_ref[...]
    old = old_ref[...]
    x = newton_step(
        x_ref[...], old - dual, summed(margin_ref), label_ref[...], blk_ref, turn_ref, hot_ref, masks
    )
    x_out[...] = x
    for peer in range(sent_ref.shape[0]):
        for i, sent in enumerate((x, dual, old)):
            sent_ref[peer, i] = sent


def full_sum(values):
    return jnp.sum(jnp.sum(values, axis=1, keepdims=True), axis=0, keepdims=True)


def consensus_kernel(came_ref, place_ref, x_ref, dual_ref, cons_ref, dual_out, sums_ref):
    groups = came_ref.shape[0] // SHARDS
    primal = change = None
    found = []
    for group in range(groups):
        peers = range(group * SHARDS, (group + 1) * SHARDS)
        solved = [came_ref[i, 0] for i in peers]
        both = [came_ref[i, 0] + came_ref[i, 1] for i in peers]
        old = came_ref[group * SHARDS, 2]
        total = both[0]
        for each in both[1:]:
            total = total + each
        averaged = total / float(SHARDS)
        cut = jnp.maximum(jnp.abs(averaged) - threshold, 0.0)
        consensus = jnp.where(averaged < 0.0, -cut, cut)
        found.append(consensus)
        squares = [(each - consensus) ** 2 for each in solved]
        for square in squares:
            primal = square if primal is None else primal + square
        moved = (consensus - old) ** 2
        change = moved if change is None else change + moved
    consensus = found[0]
    for group in range(1, groups):
        own = jnp.broadcast_to(place_ref[:1, :1], consensus.shape) == float(group)
        consensus = jnp.where(own, found[group], consensus)
    cons_ref[...] = consensus
    dual_out[...] = dual_ref[...] + x_ref[...] - consensus
    lane = lax.broadcasted_iota(jnp.int32, (1, LANES), 1)
    sums = jnp.where(
        lane == 0,
        full_sum(primal),
        jnp.where(lane == 1, float(SHARDS) * full_sum(change), 0.0),
    )
    sums_ref[...] = jnp.broadcast_to(sums, sums_ref.shape)


def finish_kernel(sums_ref, x_ref, dual_ref, cons_ref, x_out, dual_out, cons_out, norms_out, norms_ref, sems):
    pairs = ((x_ref, x_out), (dual_ref, dual_out), (cons_ref, cons_out))
    copies = [pltpu.make_async_copy(src, dst, sems.at[i]) for i, (src, dst) in enumerate(pairs)]
    for copy in copies:
        copy.start()
    sums = jnp.sqrt(jnp.sum(sums_ref[...], axis=0, keepdims=True))
    lane = lax.broadcasted_iota(jnp.int32, sums.shape, 1)
    norms_ref[...] = jnp.where(lane == 1, penalty * sums, sums)[0, :2]
    last = pltpu.make_async_copy(norms_ref, norms_out, sems.at[len(copies)])
    last.start()
    for copy in copies + [last]:
        copy.wait()


def exchanged(x, axis):
    return lax.all_to_all(x, axis, 0, 0, tiled=True)


def tables_to_sum(lines):
    far = lax.axis_size(FAR)
    parts = exchanged(lines.reshape(far, -1, LANES), FAR)
    own = jnp.sum(parts, axis=0)
    copies = jnp.broadcast_to(own[None], (lax.axis_size("feat_2") * far, *own.shape))
    return exchanged(copies, ("feat_2",) + FAR).reshape(-1, LANES)


def local(local_x, dual_var, consensus_old, blocks_data, row_index, labels):
    x = local_x[0]
    dual = dual_var[0]
    blocks = blocks_data[0]
    index = row_index[0]
    marks = labels.reshape(-1, LANES)
    lanes, size = x.shape
    rows = index.shape[1]
    near = lax.axis_size(NEAR)
    far = lax.axis_size(FAR)
    place = jnp.full((8, LANES), lax.axis_index("feat_2"), jnp.float32)
    given = (index, x, blocks, dual, consensus_old, marks)
    terms, hots, turned, place, label, index, x, blocks, dual, old = call(
        first_kernel,
        held(marks.shape),
        held((lanes, LOW, rows), jnp.bfloat16),
        held((lanes, size, rows), jnp.bfloat16),
        held(place.shape),
        held(index.shape),
        *[held(each.shape, each.dtype) for each in given[:-1]],
        in_specs=[pl.BlockSpec(memory_space=pltpu.VMEM)] + [HBM] * len(given),
        scratch_shapes=[
            pltpu.VMEM(marks.shape, marks.dtype),
            pltpu.SemaphoreType.DMA((len(given),)),
            pltpu.SemaphoreType.DMA((lanes,)),
        ],
    )(*in_vmem(place), *in_hbm(*given))
    kept = (blocks, dual, old, label)
    margins = tables_to_sum(terms)
    x, terms = call(
        middle_kernel,
        held(x.shape),
        held(marks.shape),
        scratch_shapes=[pltpu.VMEM((lanes, rows, LOW), jnp.bfloat16)],
    )(
        *in_vmem(margins, hots, turned, index, x, *kept)
    )
    margins = tables_to_sum(terms)
    x, sent = call(last_kernel, held(x.shape), held((near, 3, lanes, size)))(
        *in_vmem(margins, hots, turned, index, x, *kept)
    )
    came = exchanged(sent, NEAR)
    consensus, dual, sums = call(
        consensus_kernel, held(x.shape), held(x.shape), held((far, LANES))
    )(*in_vmem(came, place, x, dual))
    sums = exchanged(sums.reshape(far, 1, LANES), FAR).reshape(far, LANES)
    whole = jax.ShapeDtypeStruct(x.shape, jnp.float32)
    x, dual, consensus, norms = call(
        finish_kernel,
        whole,
        whole,
        whole,
        jax.ShapeDtypeStruct((2,), jnp.float32),
        out_specs=(HBM, HBM, HBM, HBM),
        scratch_shapes=[pltpu.VMEM((2,), jnp.float32), pltpu.SemaphoreType.DMA((4,))],
    )(*in_vmem(sums, x, dual, consensus))
    return (x[None], dual[None], consensus, norms)


def solution(mesh):
    if mesh.shape["feat"] == 64:
        feat = (8, 4, 2)
    else:
        feat = (mesh.shape["feat"] // 2, 1, 2)
    torus = Mesh(
        mesh.devices.reshape(*feat, mesh.shape["row"], mesh.shape["col"]), FEAT + SHARD
    )
    placed = (
        P(SHARD, FEAT, None),
        P(SHARD, FEAT, None),
        P(FEAT, None),
        P(SHARD, FEAT, None, None),
        P(SHARD, FEAT, None),
        P(SHARD, None),
    )
    return jax.shard_map(
        local,
        mesh=torus,
        in_specs=placed,
        out_specs=(P(SHARD, FEAT, None), P(SHARD, FEAT, None), P(FEAT, None), P()),
        check_vma=False,
    )
```

```python
import jax
import jax.numpy as jnp
from jax import lax
from jax.experimental import pallas as pl
from jax.experimental.pallas import tpu as pltpu
from jax.sharding import Mesh
from jax.sharding import PartitionSpec as P

CG_STEPS = 3
FEAT = ("z", "y_hi", "y_lo", "x_hi")
SHARD = ("row", "col")
NEAR = ("x_hi", "row", "col")
FAR = ("z", "y_hi", "y_lo")
ACROSS = ("x_hi", "z", "y_lo")
LANES = 128
HIGH = 64
LOW = 256
SHARDS = 4
INTERPRET = False

penalty = 1.0
damping = 0.5
threshold = 0.05


HBM = pl.BlockSpec(memory_space=pltpu.HBM)


def placed_in(space, args):
    if INTERPRET:
        return args
    return [pltpu.with_memory_space_constraint(arg, space) for arg in args]


def in_vmem(*args):
    return placed_in(pltpu.VMEM, args)


def in_hbm(*args):
    return placed_in(pltpu.HBM, args)


def held(shape, kind=jnp.float32):
    if INTERPRET:
        return jax.ShapeDtypeStruct(shape, kind)
    return pltpu.VMEM(shape, kind)


def call(kernel, *outs, **options):
    return pl.pallas_call(
        kernel,
        out_shape=outs,
        interpret=INTERPRET,
        compiler_params=pltpu.CompilerParams(vmem_limit_bytes=16 << 20),
        **options,
    )


def dot(a, b, dims):
    return lax.dot_general(a, b, (dims, ((), ())), preferred_element_type=jnp.float32)


NN = ((1,), (0,))
NT = ((1,), (1,))


def three_parts(x):
    first = x.astype(jnp.bfloat16).astype(jnp.float32)
    rest = x - first
    second = rest.astype(jnp.bfloat16).astype(jnp.float32)
    return first, second, rest - second


def low_hot(index):
    low = (index & 127) | ((index >> 13) << 7)
    places = lax.broadcasted_iota(jnp.int32, (LOW, index.shape[1]), 0)
    return jnp.where(places == low, 1.0, 0.0).astype(jnp.bfloat16)


def high_mask(index):
    high = (index >> 7) & (HIGH - 1)
    places = lax.broadcasted_iota(jnp.int32, (HIGH, index.shape[1]), 0)
    return places == high


def as_table(lines):
    return jnp.concatenate([lines[:HIGH], lines[HIGH:]], axis=1)


def spread(partial, hot_ref, masks, dims):
    parts = three_parts(partial)
    table = None
    spreads = [
        jnp.concatenate([jnp.where(mask, part[b : b + 1], 0.0) for part in parts], axis=0)
        for b, mask in enumerate(masks)
    ]
    for b, spread_rows in enumerate(spreads):
        added = dot(spread_rows.astype(jnp.bfloat16), hot_ref[b], dims)
        table = added if table is None else table + added
    return table


def put(table, out_ref):
    table = table[:HIGH] + table[HIGH : 2 * HIGH] + table[2 * HIGH :]
    table = jnp.concatenate([table[:, :LANES], table[:, LANES:]], axis=0)
    parts, copies, lines, _ = out_ref.shape
    for part in range(parts):
        for copy in range(copies):
            out_ref[part, copy] = table[part * lines : (part + 1) * lines]


def picked(found, masks):
    rows = [
        jnp.sum(jnp.where(mask, each, 0.0), axis=0, keepdims=True)
        for each, mask in zip(found, masks)
    ]
    return jnp.concatenate(rows, axis=0)


def identity_of(size):
    rows = lax.broadcasted_iota(jnp.int32, (size, size), 0)
    cols = lax.broadcasted_iota(jnp.int32, (size, size), 1)
    return jnp.where(rows == cols, 1.0, 0.0)


def as_column(line):
    size = line.shape[1]
    pieces = [
        jnp.transpose(jnp.broadcast_to(line[:, start : start + LANES], (LANES, LANES)))
        for start in range(0, size, LANES)
    ]
    return jnp.concatenate([jnp.concatenate(pieces, axis=0)] * (size // LANES), axis=1)


def newton_step(x, target, margins, labels, blk_ref, turn_ref, hot_ref, masks):
    blocks, size = x.shape
    tables = jnp.concatenate(three_parts(as_table(margins)), axis=0).astype(jnp.bfloat16)
    found = [dot(tables, hot_ref[b], NN) for b in range(blocks)]
    found = [each[:HIGH] + each[HIGH : 2 * HIGH] + each[2 * HIGH :] for each in found]
    prob = 1.0 / (1.0 + jnp.exp(-picked(found, masks)))
    misfit = (prob - labels).astype(jnp.bfloat16)
    weight = prob * (1.0 - prob)
    identity = penalty * identity_of(size)
    gradients = [dot(misfit, blk_ref[b], NN)[b : b + 1] for b in range(blocks)]
    weighted = [
        (turn_ref[b].astype(jnp.float32) * weight[b : b + 1]).astype(jnp.bfloat16)
        for b in range(blocks)
    ]
    hessians = [dot(weighted[b], blk_ref[b], NN) + identity for b in range(blocks)]
    gradient = jnp.concatenate(gradients, axis=0) + penalty * (x - target)
    delta = jnp.zeros_like(gradient)
    residual = gradient
    direction = gradient
    power = jnp.sum(residual * residual, axis=1, keepdims=True)
    for cg_step in range(CG_STEPS):
        image = jnp.concatenate(
            [
                jnp.sum(hessians[b] * as_column(direction[b : b + 1]), axis=0, keepdims=True)
                for b in range(blocks)
            ],
            axis=0,
        )
        alpha = power / jnp.sum(direction * image, axis=1, keepdims=True)
        delta = delta + alpha * direction
        residual = residual - alpha * image
        power_next = jnp.sum(residual * residual, axis=1, keepdims=True)
        direction = residual + (power_next / power) * direction
        power = power_next
    return x - damping * delta


def masks_of(idx_ref):
    return [high_mask(idx_ref[b : b + 1, :]) for b in range(idx_ref.shape[0])]


def first_kernel(place_ref, *refs):
    given, (table_ref, hot_ref, turn_ref, place_out, label_ref, *kept), scratch = refs[:6], refs[6:-3], refs[-3:]
    marks_ref, sems, block_sems = scratch
    kept = (*kept, marks_ref)
    (idx_in, x_in, blk_in, *_), (idx_ref, x_ref, blk_ref, *_) = given, kept
    copies = [
        pltpu.make_async_copy(src, dst, sems.at[i])
        for i, (src, dst) in enumerate(zip(given, kept))
        if i != 2
    ]
    blocks = [
        pltpu.make_async_copy(blk_in.at[b], blk_ref.at[b], block_sems.at[b])
        for b in range(blk_ref.shape[0])
    ]
    for copy in (copies[0], copies[1], copies[-1], *blocks, *copies[2:-1]):
        copy.start()
    place_out[...] = place_ref[...]
    copies[0].wait()
    for b in range(blk_ref.shape[0]):
        hot_ref[b] = low_hot(idx_ref[b : b + 1, :])
    masks = masks_of(idx_ref)
    copies[-1].wait()
    marks = as_table(marks_ref[...].astype(jnp.float32)).astype(jnp.bfloat16)
    found = [dot(marks, hot_ref[b], NN) for b in range(blk_ref.shape[0])]
    label_ref[...] = picked(found, masks)
    copies[1].wait()
    rounded = x_ref[...].astype(jnp.bfloat16)
    for copy in blocks:
        copy.wait()
    partial = []
    for b in range(blk_ref.shape[0]):
        turned = jnp.transpose(blk_ref[b])
        turn_ref[b] = turned
        partial.append(dot(rounded, turned, NN)[b : b + 1])
    put(spread(jnp.concatenate(partial, axis=0), hot_ref, masks, NT), table_ref)
    for copy in copies[2:-1]:
        copy.wait()


def summed(margin_ref):
    lines = LANES
    total = margin_ref[:lines]
    for start in range(lines, margin_ref.shape[0], lines):
        total = total + margin_ref[start : start + lines]
    return total


def middle_kernel(margin_ref, hot_ref, turn_ref, idx_ref, x_ref, blk_ref, dual_ref, old_ref, label_ref, x_out, out_ref, stood_ref):
    masks = masks_of(idx_ref)
    for b in range(x_ref.shape[0]):
        stood_ref[b] = jnp.transpose(hot_ref[b])
    target = old_ref[...] - dual_ref[...]
    x = newton_step(
        x_ref[...], target, summed(margin_ref), label_ref[...], blk_ref, turn_ref, hot_ref, masks
    )
    x_out[...] = x
    rounded = x.astype(jnp.bfloat16)
    partial = [dot(rounded, turn_ref[b], NN)[b : b + 1] for b in range(x.shape[0])]
    put(spread(jnp.concatenate(partial, axis=0), stood_ref, masks, NN), out_ref)


def last_kernel(
    margin_ref, hot_ref, turn_ref, idx_ref, x_ref, blk_ref, dual_ref, old_ref, label_ref, x_out, sent_ref
):
    masks = masks_of(idx_ref)
    dual = dual_ref[...]
    old = old_ref[...]
    x = newton_step(
        x_ref[...], old - dual, summed(margin_ref), label_ref[...], blk_ref, turn_ref, hot_ref, masks
    )
    x_out[...] = x
    for peer in range(sent_ref.shape[0]):
        for i, sent in enumerate((x, dual, old)):
            sent_ref[peer, i] = sent


def full_sum(values):
    return jnp.sum(jnp.sum(values, axis=1, keepdims=True), axis=0, keepdims=True)


def consensus_kernel(came_ref, place_ref, x_ref, dual_ref, cons_ref, dual_out, sums_ref):
    groups = came_ref.shape[0] // SHARDS
    primal = change = None
    found = []
    for group in range(groups):
        peers = range(group * SHARDS, (group + 1) * SHARDS)
        solved = [came_ref[i, 0] for i in peers]
        both = [came_ref[i, 0] + came_ref[i, 1] for i in peers]
        old = came_ref[group * SHARDS, 2]
        total = both[0]
        for each in both[1:]:
            total = total + each
        averaged = total / float(SHARDS)
        cut = jnp.maximum(jnp.abs(averaged) - threshold, 0.0)
        consensus = jnp.where(averaged < 0.0, -cut, cut)
        found.append(consensus)
        squares = [(each - consensus) ** 2 for each in solved]
        for square in squares:
            primal = square if primal is None else primal + square
        moved = (consensus - old) ** 2
        change = moved if change is None else change + moved
    consensus = found[0]
    for group in range(1, groups):
        own = jnp.broadcast_to(place_ref[:1, :1], consensus.shape) == float(group)
        consensus = jnp.where(own, found[group], consensus)
    cons_ref[...] = consensus
    dual_out[...] = dual_ref[...] + x_ref[...] - consensus
    lane = lax.broadcasted_iota(jnp.int32, (1, LANES), 1)
    sums = jnp.where(
        lane == 0,
        full_sum(primal),
        jnp.where(lane == 1, float(SHARDS) * full_sum(change), 0.0),
    )
    sums_ref[...] = jnp.broadcast_to(sums, sums_ref.shape)


def finish_kernel(sums_ref, x_ref, dual_ref, cons_ref, x_out, dual_out, cons_out, norms_out, norms_ref, sems):
    pairs = ((x_ref, x_out), (dual_ref, dual_out), (cons_ref, cons_out))
    copies = [pltpu.make_async_copy(src, dst, sems.at[i]) for i, (src, dst) in enumerate(pairs)]
    for copy in copies:
        copy.start()
    sums = jnp.sqrt(jnp.sum(sums_ref[...], axis=0, keepdims=True))
    lane = lax.broadcasted_iota(jnp.int32, sums.shape, 1)
    norms_ref[...] = jnp.where(lane == 1, penalty * sums, sums)[0, :2]
    last = pltpu.make_async_copy(norms_ref, norms_out, sems.at[len(copies)])
    last.start()
    for copy in copies + [last]:
        copy.wait()


def exchanged(x, axis):
    return lax.all_to_all(x, axis, 0, 0, tiled=True)


def tables_to_sum(terms):
    pieces = terms.reshape(lax.axis_size(FAR), -1, LANES)
    own = jnp.sum(exchanged(pieces, FAR), axis=0)
    copies = jnp.broadcast_to(own[None], (lax.axis_size(ACROSS), *own.shape))
    return exchanged(copies, ACROSS).reshape(-1, LANES)


def local(local_x, dual_var, consensus_old, blocks_data, row_index, labels):
    x = local_x[0]
    dual = dual_var[0]
    blocks = blocks_data[0]
    index = row_index[0]
    marks = labels.reshape(-1, LANES)
    lanes, size = x.shape
    rows = index.shape[1]
    near = lax.axis_size(NEAR)
    far = lax.axis_size(FAR)
    place = jnp.full((8, LANES), lax.axis_index("x_hi"), jnp.float32)
    zs = lax.axis_size("z")
    spread_out = held((zs, lax.axis_size("y_hi"), marks.shape[0] // zs, LANES))
    given = (index, x, blocks, dual, consensus_old, marks)
    terms, hots, turned, place, label, index, x, blocks, dual, old = call(
        first_kernel,
        spread_out,
        held((lanes, LOW, rows), jnp.bfloat16),
        held((lanes, size, rows), jnp.bfloat16),
        held(place.shape),
        held(index.shape),
        *[held(each.shape, each.dtype) for each in given[:-1]],
        in_specs=[pl.BlockSpec(memory_space=pltpu.VMEM)] + [HBM] * len(given),
        scratch_shapes=[
            pltpu.VMEM(marks.shape, marks.dtype),
            pltpu.SemaphoreType.DMA((len(given),)),
            pltpu.SemaphoreType.DMA((lanes,)),
        ],
    )(*in_vmem(place), *in_hbm(*given))
    kept = (blocks, dual, old, label)
    margins = tables_to_sum(terms)
    x, terms = call(
        middle_kernel,
        held(x.shape),
        spread_out,
        scratch_shapes=[pltpu.VMEM((lanes, rows, LOW), jnp.bfloat16)],
    )(
        *in_vmem(margins, hots, turned, index, x, *kept)
    )
    margins = tables_to_sum(terms)
    x, sent = call(last_kernel, held(x.shape), held((near, 3, lanes, size)))(
        *in_vmem(margins, hots, turned, index, x, *kept)
    )
    came = exchanged(sent, NEAR)
    consensus, dual, sums = call(
        consensus_kernel, held(x.shape), held(x.shape), held((far, LANES))
    )(*in_vmem(came, place, x, dual))
    sums = exchanged(sums.reshape(far, 1, LANES), FAR).reshape(far, LANES)
    whole = jax.ShapeDtypeStruct(x.shape, jnp.float32)
    x, dual, consensus, norms = call(
        finish_kernel,
        whole,
        whole,
        whole,
        jax.ShapeDtypeStruct((2,), jnp.float32),
        out_specs=(HBM, HBM, HBM, HBM),
        scratch_shapes=[pltpu.VMEM((2,), jnp.float32), pltpu.SemaphoreType.DMA((4,))],
    )(*in_vmem(sums, x, dual, consensus))
    return (x[None], dual[None], consensus, norms)


def solution(mesh):
    feat = {64: (8, 2, 2, 2), 16: (2, 2, 2, 2), 2: (1, 1, 1, 2)}[mesh.shape["feat"]]
    torus = Mesh(
        mesh.devices.reshape(*feat, mesh.shape["row"], mesh.shape["col"]), FEAT + SHARD
    )
    placed = (
        P(SHARD, FEAT, None),
        P(SHARD, FEAT, None),
        P(FEAT, None),
        P(SHARD, FEAT, None, None),
        P(SHARD, FEAT, None),
        P(SHARD, None),
    )
    return jax.shard_map(
        local,
        mesh=torus,
        in_specs=placed,
        out_specs=(P(SHARD, FEAT, None), P(SHARD, FEAT, None), P(FEAT, None), P()),
        check_vma=False,
    )
```

```python
import jax
import jax.numpy as jnp
from jax import lax
from jax.experimental import pallas as pl
from jax.experimental.pallas import tpu as pltpu
from jax.sharding import Mesh
from jax.sharding import PartitionSpec as P

CG_STEPS = 3
FEAT = ("z", "y_hi", "y_lo", "x_hi")
SHARD = ("row", "col")
NEAR = ("x_hi", "row", "col")
FAR = ("z", "y_hi", "y_lo")
ACROSS = ("x_hi", "z", "y_lo")
LANES = 128
HIGH = 64
LOW = 256
SHARDS = 4
INTERPRET = False

penalty = 1.0
damping = 0.5
threshold = 0.05


HBM = pl.BlockSpec(memory_space=pltpu.HBM)


def placed_in(space, args):
    if INTERPRET:
        return args
    return [pltpu.with_memory_space_constraint(arg, space) for arg in args]


def in_vmem(*args):
    return placed_in(pltpu.VMEM, args)


def in_hbm(*args):
    return placed_in(pltpu.HBM, args)


def held(shape, kind=jnp.float32):
    if INTERPRET:
        return jax.ShapeDtypeStruct(shape, kind)
    return pltpu.VMEM(shape, kind)


def call(kernel, *outs, **options):
    return pl.pallas_call(
        kernel,
        out_shape=outs,
        interpret=INTERPRET,
        compiler_params=pltpu.CompilerParams(vmem_limit_bytes=16 << 20),
        **options,
    )


def dot(a, b, dims):
    return lax.dot_general(a, b, (dims, ((), ())), preferred_element_type=jnp.float32)


NN = ((1,), (0,))
NT = ((1,), (1,))


def three_parts(x):
    first = x.astype(jnp.bfloat16).astype(jnp.float32)
    rest = x - first
    second = rest.astype(jnp.bfloat16).astype(jnp.float32)
    return first, second, rest - second


def low_hot(index):
    low = (index & 127) | ((index >> 13) << 7)
    places = lax.broadcasted_iota(jnp.int32, (LOW, index.shape[1]), 0)
    return jnp.where(places == low, 1.0, 0.0).astype(jnp.bfloat16)


def high_mask(index):
    high = (index >> 7) & (HIGH - 1)
    places = lax.broadcasted_iota(jnp.int32, (HIGH, index.shape[1]), 0)
    return places == high


def as_table(lines):
    return jnp.concatenate([lines[:HIGH], lines[HIGH:]], axis=1)


def spread(partial, hot_ref, masks, dims):
    parts = three_parts(partial)
    table = None
    spreads = [
        jnp.concatenate([jnp.where(mask, part[b : b + 1], 0.0) for part in parts], axis=0)
        for b, mask in enumerate(masks)
    ]
    for b, spread_rows in enumerate(spreads):
        added = dot(spread_rows.astype(jnp.bfloat16), hot_ref[b], dims)
        table = added if table is None else table + added
    return table


def put(table, out_ref):
    table = table[:HIGH] + table[HIGH : 2 * HIGH] + table[2 * HIGH :]
    table = jnp.concatenate([table[:, :LANES], table[:, LANES:]], axis=0)
    parts, copies, lines, _ = out_ref.shape
    for part in range(parts):
        for copy in range(copies):
            out_ref[part, copy] = table[part * lines : (part + 1) * lines]


def picked(found, masks):
    rows = [
        jnp.sum(jnp.where(mask, each, 0.0), axis=0, keepdims=True)
        for each, mask in zip(found, masks)
    ]
    return jnp.concatenate(rows, axis=0)


def identity_of(size):
    rows = lax.broadcasted_iota(jnp.int32, (size, size), 0)
    cols = lax.broadcasted_iota(jnp.int32, (size, size), 1)
    return jnp.where(rows == cols, 1.0, 0.0)


def as_column(line):
    size = line.shape[1]
    pieces = [
        jnp.transpose(jnp.broadcast_to(line[:, start : start + LANES], (LANES, LANES)))
        for start in range(0, size, LANES)
    ]
    return jnp.concatenate([jnp.concatenate(pieces, axis=0)] * (size // LANES), axis=1)


def image_of(hessians, lines):
    images = [
        jnp.sum(hessian * as_column(lines[b : b + 1]), axis=0, keepdims=True)
        for b, hessian in enumerate(hessians)
    ]
    return jnp.concatenate(images, axis=0)


def sums_of(lines):
    return jnp.sum(lines, axis=1, keepdims=True)


def newton_step(x, target, margins, labels, blk_ref, turn_ref, hot_ref, masks):
    blocks, size = x.shape
    tables = jnp.concatenate(three_parts(as_table(margins)), axis=0).astype(jnp.bfloat16)
    found = [dot(tables, hot_ref[b], NN) for b in range(blocks)]
    found = [each[:HIGH] + each[HIGH : 2 * HIGH] + each[2 * HIGH :] for each in found]
    prob = 1.0 / (1.0 + jnp.exp(-picked(found, masks)))
    misfit = (prob - labels).astype(jnp.bfloat16)
    weight = prob * (1.0 - prob)
    identity = penalty * identity_of(size)
    gradients = [dot(misfit, blk_ref[b], NN)[b : b + 1] for b in range(blocks)]
    weighted = [
        (turn_ref[b].astype(jnp.float32) * weight[b : b + 1]).astype(jnp.bfloat16)
        for b in range(blocks)
    ]
    hessians = [dot(weighted[b], blk_ref[b], NN) + identity for b in range(blocks)]
    gradient = jnp.concatenate(gradients, axis=0) + penalty * (x - target)
    residual = direction = gradient
    image = image_of(hessians, direction)
    power = sums_of(residual * residual)
    alpha = power / sums_of(direction * image)
    delta = alpha * direction
    for cg_step in range(1, CG_STEPS):
        residual = residual - alpha * image
        turned = image_of(hessians, residual)
        power_next = sums_of(residual * residual)
        beta = power_next / power
        direction = residual + beta * direction
        image = turned + beta * image
        power = power_next
        alpha = power / sums_of(direction * image)
        delta = delta + alpha * direction
    return x - damping * delta


def masks_of(idx_ref):
    return [high_mask(idx_ref[b : b + 1, :]) for b in range(idx_ref.shape[0])]


def first_kernel(place_ref, *refs):
    given, (table_ref, hot_ref, turn_ref, place_out, label_ref, *kept), scratch = refs[:6], refs[6:-3], refs[-3:]
    marks_ref, sems, block_sems = scratch
    kept = (*kept, marks_ref)
    (idx_in, x_in, blk_in, *_), (idx_ref, x_ref, blk_ref, *_) = given, kept
    copies = [
        pltpu.make_async_copy(src, dst, sems.at[i])
        for i, (src, dst) in enumerate(zip(given, kept))
        if i != 2
    ]
    blocks = [
        pltpu.make_async_copy(blk_in.at[b], blk_ref.at[b], block_sems.at[b])
        for b in range(blk_ref.shape[0])
    ]
    for copy in (copies[0], copies[1], copies[-1], *blocks, *copies[2:-1]):
        copy.start()
    place_out[...] = place_ref[...]
    for copy in (copies[0], copies[1], copies[-1], *blocks):
        copy.wait()
    for b in range(blk_ref.shape[0]):
        hot_ref[b] = low_hot(idx_ref[b : b + 1, :])
    masks = masks_of(idx_ref)
    marks = as_table(marks_ref[...].astype(jnp.float32)).astype(jnp.bfloat16)
    found = [dot(marks, hot_ref[b], NN) for b in range(blk_ref.shape[0])]
    label_ref[...] = picked(found, masks)
    rounded = x_ref[...].astype(jnp.bfloat16)
    partial = []
    for b in range(blk_ref.shape[0]):
        turned = jnp.transpose(blk_ref[b])
        turn_ref[b] = turned
        partial.append(dot(rounded, turned, NN)[b : b + 1])
    put(spread(jnp.concatenate(partial, axis=0), hot_ref, masks, NT), table_ref)
    for copy in copies[2:-1]:
        copy.wait()


def summed(margin_ref):
    lines = LANES
    total = margin_ref[:lines]
    for start in range(lines, margin_ref.shape[0], lines):
        total = total + margin_ref[start : start + lines]
    return total


def middle_kernel(margin_ref, hot_ref, turn_ref, idx_ref, x_ref, blk_ref, dual_ref, old_ref, label_ref, x_out, out_ref, stood_ref):
    masks = masks_of(idx_ref)
    for b in range(x_ref.shape[0]):
        stood_ref[b] = jnp.transpose(hot_ref[b])
    target = old_ref[...] - dual_ref[...]
    x = newton_step(
        x_ref[...], target, summed(margin_ref), label_ref[...], blk_ref, turn_ref, hot_ref, masks
    )
    x_out[...] = x
    rounded = x.astype(jnp.bfloat16)
    partial = [dot(rounded, turn_ref[b], NN)[b : b + 1] for b in range(x.shape[0])]
    put(spread(jnp.concatenate(partial, axis=0), stood_ref, masks, NN), out_ref)


def last_kernel(
    margin_ref, hot_ref, turn_ref, idx_ref, x_ref, blk_ref, dual_ref, old_ref, label_ref, x_out, sent_ref
):
    masks = masks_of(idx_ref)
    dual = dual_ref[...]
    old = old_ref[...]
    x = newton_step(
        x_ref[...], old - dual, summed(margin_ref), label_ref[...], blk_ref, turn_ref, hot_ref, masks
    )
    x_out[...] = x
    for peer in range(sent_ref.shape[0]):
        for i, sent in enumerate((x, dual, old)):
            sent_ref[peer, i] = sent


def full_sum(values):
    return jnp.sum(jnp.sum(values, axis=1, keepdims=True), axis=0, keepdims=True)


def consensus_kernel(came_ref, place_ref, x_ref, dual_ref, cons_ref, dual_out, sums_ref):
    groups = came_ref.shape[0] // SHARDS
    primal = change = None
    found = []
    for group in range(groups):
        peers = range(group * SHARDS, (group + 1) * SHARDS)
        solved = [came_ref[i, 0] for i in peers]
        both = [came_ref[i, 0] + came_ref[i, 1] for i in peers]
        old = came_ref[group * SHARDS, 2]
        total = both[0]
        for each in both[1:]:
            total = total + each
        averaged = total / float(SHARDS)
        cut = jnp.maximum(jnp.abs(averaged) - threshold, 0.0)
        consensus = jnp.where(averaged < 0.0, -cut, cut)
        found.append(consensus)
        squares = [(each - consensus) ** 2 for each in solved]
        for square in squares:
            primal = square if primal is None else primal + square
        moved = (consensus - old) ** 2
        change = moved if change is None else change + moved
    consensus = found[0]
    for group in range(1, groups):
        own = jnp.broadcast_to(place_ref[:1, :1], consensus.shape) == float(group)
        consensus = jnp.where(own, found[group], consensus)
    cons_ref[...] = consensus
    dual_out[...] = dual_ref[...] + x_ref[...] - consensus
    lane = lax.broadcasted_iota(jnp.int32, (1, LANES), 1)
    sums = jnp.where(
        lane == 0,
        full_sum(primal),
        jnp.where(lane == 1, float(SHARDS) * full_sum(change), 0.0),
    )
    sums_ref[...] = jnp.broadcast_to(sums, sums_ref.shape)


def finish_kernel(sums_ref, x_ref, dual_ref, cons_ref, x_out, dual_out, cons_out, norms_out, norms_ref, sems):
    pairs = ((x_ref, x_out), (dual_ref, dual_out), (cons_ref, cons_out))
    copies = [pltpu.make_async_copy(src, dst, sems.at[i]) for i, (src, dst) in enumerate(pairs)]
    for copy in copies:
        copy.start()
    sums = jnp.sqrt(jnp.sum(sums_ref[...], axis=0, keepdims=True))
    lane = lax.broadcasted_iota(jnp.int32, sums.shape, 1)
    norms_ref[...] = jnp.where(lane == 1, penalty * sums, sums)[0, :2]
    last = pltpu.make_async_copy(norms_ref, norms_out, sems.at[len(copies)])
    last.start()
    for copy in copies + [last]:
        copy.wait()


def exchanged(x, axis):
    return lax.all_to_all(x, axis, 0, 0, tiled=True)


def tables_to_sum(terms):
    pieces = terms.reshape(lax.axis_size(FAR), -1, LANES)
    own = jnp.sum(exchanged(pieces, FAR), axis=0)
    copies = jnp.broadcast_to(own[None], (lax.axis_size(ACROSS), *own.shape))
    return exchanged(copies, ACROSS).reshape(-1, LANES)


def local(local_x, dual_var, consensus_old, blocks_data, row_index, labels):
    x = local_x[0]
    dual = dual_var[0]
    blocks = blocks_data[0]
    index = row_index[0]
    marks = labels.reshape(-1, LANES)
    lanes, size = x.shape
    rows = index.shape[1]
    near = lax.axis_size(NEAR)
    far = lax.axis_size(FAR)
    place = jnp.full((8, LANES), lax.axis_index("x_hi"), jnp.float32)
    zs = lax.axis_size("z")
    spread_out = held((zs, lax.axis_size("y_hi"), marks.shape[0] // zs, LANES))
    given = (index, x, blocks, dual, consensus_old, marks)
    terms, hots, turned, place, label, index, x, blocks, dual, old = call(
        first_kernel,
        spread_out,
        held((lanes, LOW, rows), jnp.bfloat16),
        held((lanes, size, rows), jnp.bfloat16),
        held(place.shape),
        held(index.shape),
        *[held(each.shape, each.dtype) for each in given[:-1]],
        in_specs=[pl.BlockSpec(memory_space=pltpu.VMEM)] + [HBM] * len(given),
        scratch_shapes=[
            pltpu.VMEM(marks.shape, marks.dtype),
            pltpu.SemaphoreType.DMA((len(given),)),
            pltpu.SemaphoreType.DMA((lanes,)),
        ],
    )(*in_vmem(place), *in_hbm(*given))
    kept = (blocks, dual, old, label)
    margins = tables_to_sum(terms)
    x, terms = call(
        middle_kernel,
        held(x.shape),
        spread_out,
        scratch_shapes=[pltpu.VMEM((lanes, rows, LOW), jnp.bfloat16)],
    )(
        *in_vmem(margins, hots, turned, index, x, *kept)
    )
    margins = tables_to_sum(terms)
    x, sent = call(last_kernel, held(x.shape), held((near, 3, lanes, size)))(
        *in_vmem(margins, hots, turned, index, x, *kept)
    )
    came = exchanged(sent, NEAR)
    consensus, dual, sums = call(
        consensus_kernel, held(x.shape), held(x.shape), held((far, LANES))
    )(*in_vmem(came, place, x, dual))
    sums = exchanged(sums.reshape(far, 1, LANES), FAR).reshape(far, LANES)
    whole = jax.ShapeDtypeStruct(x.shape, jnp.float32)
    x, dual, consensus, norms = call(
        finish_kernel,
        whole,
        whole,
        whole,
        jax.ShapeDtypeStruct((2,), jnp.float32),
        out_specs=(HBM, HBM, HBM, HBM),
        scratch_shapes=[pltpu.VMEM((2,), jnp.float32), pltpu.SemaphoreType.DMA((4,))],
    )(*in_vmem(sums, x, dual, consensus))
    return (x[None], dual[None], consensus, norms)


def solution(mesh):
    feat = {64: (8, 2, 2, 2), 16: (2, 2, 2, 2), 2: (1, 1, 1, 2)}[mesh.shape["feat"]]
    torus = Mesh(
        mesh.devices.reshape(*feat, mesh.shape["row"], mesh.shape["col"]), FEAT + SHARD
    )
    placed = (
        P(SHARD, FEAT, None),
        P(SHARD, FEAT, None),
        P(FEAT, None),
        P(SHARD, FEAT, None, None),
        P(SHARD, FEAT, None),
        P(SHARD, None),
    )
    return jax.shard_map(
        local,
        mesh=torus,
        in_specs=placed,
        out_specs=(P(SHARD, FEAT, None), P(SHARD, FEAT, None), P(FEAT, None), P()),
        check_vma=False,
    )
```

```python
import jax
import jax.numpy as jnp
from jax import lax
from jax.experimental import pallas as pl
from jax.experimental.pallas import tpu as pltpu
from jax.sharding import Mesh
from jax.sharding import PartitionSpec as P

CG_STEPS = 3
FEAT = ("z", "y_hi", "y_lo", "x_hi")
SHARD = ("row", "col")
NEAR = ("x_hi", "row", "col")
FAR = ("z", "y_hi", "y_lo")
ACROSS = ("x_hi", "z", "y_lo")
LANES = 128
HIGH = 64
LOW = 256
SHARDS = 4
INTERPRET = False

penalty = 1.0
damping = 0.5
threshold = 0.05


HBM = pl.BlockSpec(memory_space=pltpu.HBM)


def placed_in(space, args):
    if INTERPRET:
        return args
    return [pltpu.with_memory_space_constraint(arg, space) for arg in args]


def in_vmem(*args):
    return placed_in(pltpu.VMEM, args)


def in_hbm(*args):
    return placed_in(pltpu.HBM, args)


def held(shape, kind=jnp.float32):
    if INTERPRET:
        return jax.ShapeDtypeStruct(shape, kind)
    return pltpu.VMEM(shape, kind)


def call(kernel, *outs, **options):
    return pl.pallas_call(
        kernel,
        out_shape=outs,
        interpret=INTERPRET,
        compiler_params=pltpu.CompilerParams(vmem_limit_bytes=16 << 20),
        **options,
    )


def dot(a, b, dims):
    return lax.dot_general(a, b, (dims, ((), ())), preferred_element_type=jnp.float32)


NN = ((1,), (0,))
NT = ((1,), (1,))


def three_parts(x):
    first = x.astype(jnp.bfloat16).astype(jnp.float32)
    rest = x - first
    second = rest.astype(jnp.bfloat16).astype(jnp.float32)
    return first, second, rest - second


def low_hot(index):
    low = (index & 127) | ((index >> 13) << 7)
    places = lax.broadcasted_iota(jnp.int32, (LOW, index.shape[1]), 0)
    return jnp.where(places == low, 1.0, 0.0).astype(jnp.bfloat16)


def high_mask(index):
    high = (index >> 7) & (HIGH - 1)
    places = lax.broadcasted_iota(jnp.int32, (HIGH, index.shape[1]), 0)
    return places == high


def as_table(lines):
    return jnp.concatenate([lines[:HIGH], lines[HIGH:]], axis=1)


def spread(partial, hot_ref, masks, dims):
    parts = three_parts(partial)
    table = None
    spreads = [
        jnp.concatenate([jnp.where(mask, part[b : b + 1], 0.0) for part in parts], axis=0)
        for b, mask in enumerate(masks)
    ]
    for b, spread_rows in enumerate(spreads):
        added = dot(spread_rows.astype(jnp.bfloat16), hot_ref[b], dims)
        table = added if table is None else table + added
    return table


def put(table, out_ref):
    table = table[:HIGH] + table[HIGH : 2 * HIGH] + table[2 * HIGH :]
    table = jnp.concatenate([table[:, :LANES], table[:, LANES:]], axis=0)
    parts, copies, lines, _ = out_ref.shape
    for part in range(parts):
        for copy in range(copies):
            out_ref[part, copy] = table[part * lines : (part + 1) * lines]


def picked(found, masks):
    rows = [
        jnp.sum(jnp.where(mask, each, 0.0), axis=0, keepdims=True)
        for each, mask in zip(found, masks)
    ]
    return jnp.concatenate(rows, axis=0)


def identity_of(size):
    rows = lax.broadcasted_iota(jnp.int32, (size, size), 0)
    cols = lax.broadcasted_iota(jnp.int32, (size, size), 1)
    return jnp.where(rows == cols, 1.0, 0.0)


def as_column(line):
    size = line.shape[1]
    pieces = [
        jnp.transpose(jnp.broadcast_to(line[:, start : start + LANES], (LANES, LANES)))
        for start in range(0, size, LANES)
    ]
    return jnp.concatenate([jnp.concatenate(pieces, axis=0)] * (size // LANES), axis=1)


def image_of(hessians, lines):
    images = [
        jnp.sum(hessian * as_column(lines[b : b + 1]), axis=0, keepdims=True)
        for b, hessian in enumerate(hessians)
    ]
    return jnp.concatenate(images, axis=0)


def sums_of(lines):
    return jnp.sum(lines, axis=1, keepdims=True)


def newton_step(x, target, margins, labels, blk_ref, turn_ref, hot_ref, masks):
    blocks, size = x.shape
    tables = jnp.concatenate(three_parts(as_table(margins)), axis=0).astype(jnp.bfloat16)
    found = [dot(tables, hot_ref[b], NN) for b in range(blocks)]
    found = [each[:HIGH] + each[HIGH : 2 * HIGH] + each[2 * HIGH :] for each in found]
    prob = 1.0 / (1.0 + jnp.exp(-picked(found, masks)))
    misfit = (prob - labels).astype(jnp.bfloat16)
    weight = prob * (1.0 - prob)
    identity = penalty * identity_of(size)
    gradients = [dot(misfit, blk_ref[b], NN)[b : b + 1] for b in range(blocks)]
    weighted = [
        (turn_ref[b].astype(jnp.float32) * weight[b : b + 1]).astype(jnp.bfloat16)
        for b in range(blocks)
    ]
    hessians = [dot(weighted[b], blk_ref[b], NN) + identity for b in range(blocks)]
    gradient = jnp.concatenate(gradients, axis=0) + penalty * (x - target)
    residual = direction = gradient
    image = image_of(hessians, direction)
    power = sums_of(residual * residual)
    alpha = power / sums_of(direction * image)
    delta = alpha * direction
    for cg_step in range(1, CG_STEPS):
        residual = residual - alpha * image
        turned = image_of(hessians, residual)
        power_next = sums_of(residual * residual)
        beta = power_next / power
        direction = residual + beta * direction
        image = turned + beta * image
        power = power_next
        alpha = power / sums_of(direction * image)
        delta = delta + alpha * direction
    return x - damping * delta


def masks_of(idx_ref):
    return [high_mask(idx_ref[b : b + 1, :]) for b in range(idx_ref.shape[0])]


def first_kernel(place_ref, *refs):
    given, (table_ref, hot_ref, turn_ref, place_out, *kept), (sems, block_sems) = refs[:6], refs[6:-2], refs[-2:]
    (idx_in, x_in, blk_in, *_), (idx_ref, x_ref, blk_ref, *_) = given, kept
    copies = [
        pltpu.make_async_copy(src, dst, sems.at[i])
        for i, (src, dst) in enumerate(zip(given, kept))
        if i != 2
    ]
    blocks = [
        pltpu.make_async_copy(blk_in.at[b], blk_ref.at[b], block_sems.at[b])
        for b in range(blk_ref.shape[0])
    ]
    for copy in (*copies[:2], *blocks, *copies[2:]):
        copy.start()
    place_out[...] = place_ref[...]
    copies[0].wait()
    for b in range(blk_ref.shape[0]):
        hot_ref[b] = low_hot(idx_ref[b : b + 1, :])
    masks = masks_of(idx_ref)
    copies[1].wait()
    for copy in blocks:
        copy.wait()
    rounded = x_ref[...].astype(jnp.bfloat16)
    partial = []
    for b in range(blk_ref.shape[0]):
        turned = jnp.transpose(blk_ref[b])
        turn_ref[b] = turned
        partial.append(dot(rounded, turned, NN)[b : b + 1])
    put(spread(jnp.concatenate(partial, axis=0), hot_ref, masks, NT), table_ref)
    for copy in copies[2:]:
        copy.wait()


def summed(margin_ref):
    lines = LANES
    total = margin_ref[:lines]
    for start in range(lines, margin_ref.shape[0], lines):
        total = total + margin_ref[start : start + lines]
    return total


def middle_kernel(margin_ref, hot_ref, turn_ref, idx_ref, x_ref, blk_ref, dual_ref, old_ref, marks_ref, x_out, out_ref, label_ref, stood_ref):
    masks = masks_of(idx_ref)
    marks = as_table(marks_ref[...].astype(jnp.float32)).astype(jnp.bfloat16)
    label_ref[...] = picked([dot(marks, hot_ref[b], NN) for b in range(x_ref.shape[0])], masks)
    for b in range(x_ref.shape[0]):
        stood_ref[b] = jnp.transpose(hot_ref[b])
    target = old_ref[...] - dual_ref[...]
    x = newton_step(
        x_ref[...], target, summed(margin_ref), label_ref[...], blk_ref, turn_ref, hot_ref, masks
    )
    x_out[...] = x
    rounded = x.astype(jnp.bfloat16)
    partial = [dot(rounded, turn_ref[b], NN)[b : b + 1] for b in range(x.shape[0])]
    put(spread(jnp.concatenate(partial, axis=0), stood_ref, masks, NN), out_ref)


def last_kernel(
    margin_ref, hot_ref, turn_ref, idx_ref, x_ref, blk_ref, dual_ref, old_ref, label_ref, x_out, sent_ref
):
    masks = masks_of(idx_ref)
    dual = dual_ref[...]
    old = old_ref[...]
    x = newton_step(
        x_ref[...], old - dual, summed(margin_ref), label_ref[...], blk_ref, turn_ref, hot_ref, masks
    )
    x_out[...] = x
    for peer in range(sent_ref.shape[0]):
        for i, sent in enumerate((x, dual, old)):
            sent_ref[peer, i] = sent


def full_sum(values):
    return jnp.sum(jnp.sum(values, axis=1, keepdims=True), axis=0, keepdims=True)


def consensus_kernel(came_ref, place_ref, x_ref, dual_ref, cons_ref, dual_out, sums_ref):
    groups = came_ref.shape[0] // SHARDS
    primal = change = None
    found = []
    for group in range(groups):
        peers = range(group * SHARDS, (group + 1) * SHARDS)
        solved = [came_ref[i, 0] for i in peers]
        both = [came_ref[i, 0] + came_ref[i, 1] for i in peers]
        old = came_ref[group * SHARDS, 2]
        total = both[0]
        for each in both[1:]:
            total = total + each
        averaged = total / float(SHARDS)
        cut = jnp.maximum(jnp.abs(averaged) - threshold, 0.0)
        consensus = jnp.where(averaged < 0.0, -cut, cut)
        found.append(consensus)
        squares = [(each - consensus) ** 2 for each in solved]
        for square in squares:
            primal = square if primal is None else primal + square
        moved = (consensus - old) ** 2
        change = moved if change is None else change + moved
    consensus = found[0]
    for group in range(1, groups):
        own = jnp.broadcast_to(place_ref[:1, :1], consensus.shape) == float(group)
        consensus = jnp.where(own, found[group], consensus)
    cons_ref[...] = consensus
    dual_out[...] = dual_ref[...] + x_ref[...] - consensus
    lane = lax.broadcasted_iota(jnp.int32, (1, LANES), 1)
    sums = jnp.where(
        lane == 0,
        full_sum(primal),
        jnp.where(lane == 1, float(SHARDS) * full_sum(change), 0.0),
    )
    sums_ref[...] = jnp.broadcast_to(sums, sums_ref.shape)


def finish_kernel(sums_ref, x_ref, dual_ref, cons_ref, x_out, dual_out, cons_out, norms_out, norms_ref, sems):
    pairs = ((x_ref, x_out), (dual_ref, dual_out), (cons_ref, cons_out))
    copies = [pltpu.make_async_copy(src, dst, sems.at[i]) for i, (src, dst) in enumerate(pairs)]
    for copy in copies:
        copy.start()
    sums = jnp.sqrt(jnp.sum(sums_ref[...], axis=0, keepdims=True))
    lane = lax.broadcasted_iota(jnp.int32, sums.shape, 1)
    norms_ref[...] = jnp.where(lane == 1, penalty * sums, sums)[0, :2]
    last = pltpu.make_async_copy(norms_ref, norms_out, sems.at[len(copies)])
    last.start()
    for copy in copies + [last]:
        copy.wait()


def exchanged(x, axis):
    return lax.all_to_all(x, axis, 0, 0, tiled=True)


def tables_to_sum(terms):
    pieces = terms.reshape(lax.axis_size(FAR), -1, LANES)
    own = jnp.sum(exchanged(pieces, FAR), axis=0)
    copies = jnp.broadcast_to(own[None], (lax.axis_size(ACROSS), *own.shape))
    return exchanged(copies, ACROSS).reshape(-1, LANES)


def local(local_x, dual_var, consensus_old, blocks_data, row_index, labels):
    x = local_x[0]
    dual = dual_var[0]
    blocks = blocks_data[0]
    index = row_index[0]
    marks = labels.reshape(-1, LANES)
    lanes, size = x.shape
    rows = index.shape[1]
    near = lax.axis_size(NEAR)
    far = lax.axis_size(FAR)
    place = jnp.full((8, LANES), lax.axis_index("x_hi"), jnp.float32)
    zs = lax.axis_size("z")
    spread_out = held((zs, lax.axis_size("y_hi"), marks.shape[0] // zs, LANES))
    given = (index, x, blocks, dual, consensus_old, marks)
    terms, hots, turned, place, index, x, blocks, dual, old, marks = call(
        first_kernel,
        spread_out,
        held((lanes, LOW, rows), jnp.bfloat16),
        held((lanes, size, rows), jnp.bfloat16),
        held(place.shape),
        *[held(each.shape, each.dtype) for each in given],
        in_specs=[pl.BlockSpec(memory_space=pltpu.VMEM)] + [HBM] * len(given),
        scratch_shapes=[
            pltpu.SemaphoreType.DMA((len(given),)),
            pltpu.SemaphoreType.DMA((lanes,)),
        ],
    )(*in_vmem(place), *in_hbm(*given))
    kept = (blocks, dual, old)
    margins = tables_to_sum(terms)
    x, terms, label = call(
        middle_kernel,
        held(x.shape),
        spread_out,
        held(index.shape),
        scratch_shapes=[pltpu.VMEM((lanes, rows, LOW), jnp.bfloat16)],
    )(
        *in_vmem(margins, hots, turned, index, x, *kept, marks)
    )
    margins = tables_to_sum(terms)
    x, sent = call(last_kernel, held(x.shape), held((near, 3, lanes, size)))(
        *in_vmem(margins, hots, turned, index, x, *kept, label)
    )
    came = exchanged(sent, NEAR)
    consensus, dual, sums = call(
        consensus_kernel, held(x.shape), held(x.shape), held((far, LANES))
    )(*in_vmem(came, place, x, dual))
    sums = exchanged(sums.reshape(far, 1, LANES), FAR).reshape(far, LANES)
    whole = jax.ShapeDtypeStruct(x.shape, jnp.float32)
    x, dual, consensus, norms = call(
        finish_kernel,
        whole,
        whole,
        whole,
        jax.ShapeDtypeStruct((2,), jnp.float32),
        out_specs=(HBM, HBM, HBM, HBM),
        scratch_shapes=[pltpu.VMEM((2,), jnp.float32), pltpu.SemaphoreType.DMA((4,))],
    )(*in_vmem(sums, x, dual, consensus))
    return (x[None], dual[None], consensus, norms)


def solution(mesh):
    feat = {64: (8, 2, 2, 2), 16: (2, 2, 2, 2), 2: (1, 1, 1, 2)}[mesh.shape["feat"]]
    torus = Mesh(
        mesh.devices.reshape(*feat, mesh.shape["row"], mesh.shape["col"]), FEAT + SHARD
    )
    placed = (
        P(SHARD, FEAT, None),
        P(SHARD, FEAT, None),
        P(FEAT, None),
        P(SHARD, FEAT, None, None),
        P(SHARD, FEAT, None),
        P(SHARD, None),
    )
    return jax.shard_map(
        local,
        mesh=torus,
        in_specs=placed,
        out_specs=(P(SHARD, FEAT, None), P(SHARD, FEAT, None), P(FEAT, None), P()),
        check_vma=False,
    )
```

```python
import jax
import jax.numpy as jnp
from jax import lax
from jax.experimental import pallas as pl
from jax.experimental.pallas import tpu as pltpu
from jax.sharding import Mesh
from jax.sharding import PartitionSpec as P

CG_STEPS = 3
FEAT = ("z", "y_hi", "y_lo", "x_hi")
SHARD = ("row", "col")
NEAR = ("x_hi", "row", "col")
FAR = ("z", "y_hi", "y_lo")
ACROSS = ("x_hi", "z", "y_lo")
LANES = 128
HIGH = 64
LOW = 256
SHARDS = 4
INTERPRET = False

penalty = 1.0
damping = 0.5
threshold = 0.05


HBM = pl.BlockSpec(memory_space=pltpu.HBM)


def placed_in(space, args):
    if INTERPRET:
        return args
    return [pltpu.with_memory_space_constraint(arg, space) for arg in args]


def in_vmem(*args):
    return placed_in(pltpu.VMEM, args)


def in_hbm(*args):
    return placed_in(pltpu.HBM, args)


def held(shape, kind=jnp.float32):
    if INTERPRET:
        return jax.ShapeDtypeStruct(shape, kind)
    return pltpu.VMEM(shape, kind)


def call(kernel, *outs, **options):
    return pl.pallas_call(
        kernel,
        out_shape=outs,
        interpret=INTERPRET,
        compiler_params=pltpu.CompilerParams(vmem_limit_bytes=16 << 20),
        **options,
    )


def dot(a, b, dims):
    return lax.dot_general(a, b, (dims, ((), ())), preferred_element_type=jnp.float32)


NN = ((1,), (0,))
NT = ((1,), (1,))


def three_parts(x):
    first = x.astype(jnp.bfloat16).astype(jnp.float32)
    rest = x - first
    second = rest.astype(jnp.bfloat16).astype(jnp.float32)
    return first, second, rest - second


def low_hot(index):
    low = (index & 127) | ((index >> 13) << 7)
    places = lax.broadcasted_iota(jnp.int32, (LOW, index.shape[1]), 0)
    return jnp.where(places == low, 1.0, 0.0).astype(jnp.bfloat16)


def high_mask(index):
    high = (index >> 7) & (HIGH - 1)
    places = lax.broadcasted_iota(jnp.int32, (HIGH, index.shape[1]), 0)
    return places == high


def as_table(lines):
    return jnp.concatenate([lines[:HIGH], lines[HIGH:]], axis=1)


def spread(partial, hot_ref, masks, dims):
    parts = three_parts(partial)
    table = None
    spreads = [
        jnp.concatenate([jnp.where(mask, part[b : b + 1], 0.0) for part in parts], axis=0)
        for b, mask in enumerate(masks)
    ]
    for b, spread_rows in enumerate(spreads):
        added = dot(spread_rows.astype(jnp.bfloat16), hot_ref[b], dims)
        table = added if table is None else table + added
    return table


def put(table, out_ref):
    table = table[:HIGH] + table[HIGH : 2 * HIGH] + table[2 * HIGH :]
    table = jnp.concatenate([table[:, :LANES], table[:, LANES:]], axis=0)
    parts, copies, lines, _ = out_ref.shape
    for part in range(parts):
        for copy in range(copies):
            out_ref[part, copy] = table[part * lines : (part + 1) * lines]


def picked(found, masks):
    rows = [
        jnp.sum(jnp.where(mask, each, 0.0), axis=0, keepdims=True)
        for each, mask in zip(found, masks)
    ]
    return jnp.concatenate(rows, axis=0)


def identity_of(size):
    rows = lax.broadcasted_iota(jnp.int32, (size, size), 0)
    cols = lax.broadcasted_iota(jnp.int32, (size, size), 1)
    return jnp.where(rows == cols, 1.0, 0.0)


def as_column(line):
    size = line.shape[1]
    pieces = [
        jnp.transpose(jnp.broadcast_to(line[:, start : start + LANES], (LANES, LANES)))
        for start in range(0, size, LANES)
    ]
    return jnp.concatenate([jnp.concatenate(pieces, axis=0)] * (size // LANES), axis=1)


def image_of(hessians, lines):
    images = [
        jnp.sum(hessian * as_column(lines[b : b + 1]), axis=0, keepdims=True)
        for b, hessian in enumerate(hessians)
    ]
    return jnp.concatenate(images, axis=0)


def sums_of(lines):
    return jnp.sum(lines, axis=1, keepdims=True)


def newton_step(x, target, margins, label_ref, blk_ref, turn_ref, hot_ref, masks, marks_ref=None):
    blocks, size = x.shape
    tables = three_parts(as_table(margins))
    if marks_ref is not None:
        tables += (as_table(marks_ref[...].astype(jnp.float32)),)
    tables = jnp.concatenate(tables, axis=0).astype(jnp.bfloat16)
    found = [dot(tables, hot_ref[b], NN) for b in range(blocks)]
    if marks_ref is not None:
        label_ref[...] = picked([each[3 * HIGH :] for each in found], masks)
    labels = label_ref[...]
    found = [each[:HIGH] + each[HIGH : 2 * HIGH] + each[2 * HIGH : 3 * HIGH] for each in found]
    prob = 1.0 / (1.0 + jnp.exp(-picked(found, masks)))
    misfit = (prob - labels).astype(jnp.bfloat16)
    weight = prob * (1.0 - prob)
    identity = penalty * identity_of(size)
    gradients = [dot(misfit, blk_ref[b], NN)[b : b + 1] for b in range(blocks)]
    weighted = [
        (turn_ref[b].astype(jnp.float32) * weight[b : b + 1]).astype(jnp.bfloat16)
        for b in range(blocks)
    ]
    hessians = [dot(weighted[b], blk_ref[b], NN) + identity for b in range(blocks)]
    gradient = jnp.concatenate(gradients, axis=0) + penalty * (x - target)
    residual = direction = gradient
    image = image_of(hessians, direction)
    power = sums_of(residual * residual)
    alpha = power / sums_of(direction * image)
    delta = alpha * direction
    for cg_step in range(1, CG_STEPS):
        residual = residual - alpha * image
        turned = image_of(hessians, residual)
        power_next = sums_of(residual * residual)
        beta = power_next / power
        direction = residual + beta * direction
        image = turned + beta * image
        power = power_next
        alpha = power / sums_of(direction * image)
        delta = delta + alpha * direction
    return x - damping * delta


def masks_of(idx_ref):
    return [high_mask(idx_ref[b : b + 1, :]) for b in range(idx_ref.shape[0])]


def first_kernel(place_ref, *refs):
    given, (table_ref, hot_ref, turn_ref, place_out, *kept), (sems, block_sems) = refs[:6], refs[6:-2], refs[-2:]
    (idx_in, x_in, blk_in, *_), (idx_ref, x_ref, blk_ref, *_) = given, kept
    copies = [
        pltpu.make_async_copy(src, dst, sems.at[i])
        for i, (src, dst) in enumerate(zip(given, kept))
        if i != 2
    ]
    blocks = [
        pltpu.make_async_copy(blk_in.at[b], blk_ref.at[b], block_sems.at[b])
        for b in range(blk_ref.shape[0])
    ]
    for copy in (*copies[:2], *blocks, *copies[2:]):
        copy.start()
    place_out[...] = place_ref[...]
    copies[0].wait()
    for b in range(blk_ref.shape[0]):
        hot_ref[b] = low_hot(idx_ref[b : b + 1, :])
    masks = masks_of(idx_ref)
    copies[1].wait()
    for copy in blocks:
        copy.wait()
    rounded = x_ref[...].astype(jnp.bfloat16)
    partial = []
    for b in range(blk_ref.shape[0]):
        turned = jnp.transpose(blk_ref[b])
        turn_ref[b] = turned
        partial.append(dot(rounded, turned, NN)[b : b + 1])
    put(spread(jnp.concatenate(partial, axis=0), hot_ref, masks, NT), table_ref)
    for copy in copies[2:]:
        copy.wait()


def summed(margin_ref):
    lines = LANES
    total = margin_ref[:lines]
    for start in range(lines, margin_ref.shape[0], lines):
        total = total + margin_ref[start : start + lines]
    return total


def middle_kernel(margin_ref, hot_ref, turn_ref, idx_ref, x_ref, blk_ref, dual_ref, old_ref, marks_ref, x_out, out_ref, label_ref, stood_ref):
    masks = masks_of(idx_ref)
    for b in range(x_ref.shape[0]):
        stood_ref[b] = jnp.transpose(hot_ref[b])
    target = old_ref[...] - dual_ref[...]
    x = newton_step(
        x_ref[...], target, summed(margin_ref), label_ref, blk_ref, turn_ref, hot_ref, masks, marks_ref
    )
    x_out[...] = x
    rounded = x.astype(jnp.bfloat16)
    partial = [dot(rounded, turn_ref[b], NN)[b : b + 1] for b in range(x.shape[0])]
    put(spread(jnp.concatenate(partial, axis=0), stood_ref, masks, NN), out_ref)


def last_kernel(
    margin_ref, hot_ref, turn_ref, idx_ref, x_ref, blk_ref, dual_ref, old_ref, label_ref, x_out, sent_ref
):
    masks = masks_of(idx_ref)
    dual = dual_ref[...]
    old = old_ref[...]
    x = newton_step(
        x_ref[...], old - dual, summed(margin_ref), label_ref, blk_ref, turn_ref, hot_ref, masks
    )
    x_out[...] = x
    for peer in range(sent_ref.shape[0]):
        for i, sent in enumerate((x, dual, old)):
            sent_ref[peer, i] = sent


def full_sum(values):
    return jnp.sum(jnp.sum(values, axis=1, keepdims=True), axis=0, keepdims=True)


def consensus_kernel(came_ref, place_ref, x_ref, dual_ref, cons_ref, dual_out, sums_ref):
    groups = came_ref.shape[0] // SHARDS
    primal = change = None
    found = []
    for group in range(groups):
        peers = range(group * SHARDS, (group + 1) * SHARDS)
        solved = [came_ref[i, 0] for i in peers]
        both = [came_ref[i, 0] + came_ref[i, 1] for i in peers]
        old = came_ref[group * SHARDS, 2]
        total = both[0]
        for each in both[1:]:
            total = total + each
        averaged = total / float(SHARDS)
        cut = jnp.maximum(jnp.abs(averaged) - threshold, 0.0)
        consensus = jnp.where(averaged < 0.0, -cut, cut)
        found.append(consensus)
        squares = [(each - consensus) ** 2 for each in solved]
        for square in squares:
            primal = square if primal is None else primal + square
        moved = (consensus - old) ** 2
        change = moved if change is None else change + moved
    consensus = found[0]
    for group in range(1, groups):
        own = jnp.broadcast_to(place_ref[:1, :1], consensus.shape) == float(group)
        consensus = jnp.where(own, found[group], consensus)
    cons_ref[...] = consensus
    dual_out[...] = dual_ref[...] + x_ref[...] - consensus
    lane = lax.broadcasted_iota(jnp.int32, (1, LANES), 1)
    sums = jnp.where(
        lane == 0,
        full_sum(primal),
        jnp.where(lane == 1, float(SHARDS) * full_sum(change), 0.0),
    )
    sums_ref[...] = jnp.broadcast_to(sums, sums_ref.shape)


def finish_kernel(sums_ref, x_ref, dual_ref, cons_ref, x_out, dual_out, cons_out, norms_out, norms_ref, sems):
    pairs = ((x_ref, x_out), (dual_ref, dual_out), (cons_ref, cons_out))
    copies = [pltpu.make_async_copy(src, dst, sems.at[i]) for i, (src, dst) in enumerate(pairs)]
    for copy in copies:
        copy.start()
    sums = jnp.sqrt(jnp.sum(sums_ref[...], axis=0, keepdims=True))
    lane = lax.broadcasted_iota(jnp.int32, sums.shape, 1)
    norms_ref[...] = jnp.where(lane == 1, penalty * sums, sums)[0, :2]
    last = pltpu.make_async_copy(norms_ref, norms_out, sems.at[len(copies)])
    last.start()
    for copy in copies + [last]:
        copy.wait()


def exchanged(x, axis):
    return lax.all_to_all(x, axis, 0, 0, tiled=True)


def tables_to_sum(terms):
    pieces = terms.reshape(lax.axis_size(FAR), -1, LANES)
    own = jnp.sum(exchanged(pieces, FAR), axis=0)
    copies = jnp.broadcast_to(own[None], (lax.axis_size(ACROSS), *own.shape))
    return exchanged(copies, ACROSS).reshape(-1, LANES)


def local(local_x, dual_var, consensus_old, blocks_data, row_index, labels):
    x = local_x[0]
    dual = dual_var[0]
    blocks = blocks_data[0]
    index = row_index[0]
    marks = labels.reshape(-1, LANES)
    lanes, size = x.shape
    rows = index.shape[1]
    near = lax.axis_size(NEAR)
    far = lax.axis_size(FAR)
    place = jnp.full((8, LANES), lax.axis_index("x_hi"), jnp.float32)
    zs = lax.axis_size("z")
    spread_out = held((zs, lax.axis_size("y_hi"), marks.shape[0] // zs, LANES))
    given = (index, x, blocks, dual, consensus_old, marks)
    terms, hots, turned, place, index, x, blocks, dual, old, marks = call(
        first_kernel,
        spread_out,
        held((lanes, LOW, rows), jnp.bfloat16),
        held((lanes, size, rows), jnp.bfloat16),
        held(place.shape),
        *[held(each.shape, each.dtype) for each in given],
        in_specs=[pl.BlockSpec(memory_space=pltpu.VMEM)] + [HBM] * len(given),
        scratch_shapes=[
            pltpu.SemaphoreType.DMA((len(given),)),
            pltpu.SemaphoreType.DMA((lanes,)),
        ],
    )(*in_vmem(place), *in_hbm(*given))
    kept = (blocks, dual, old)
    margins = tables_to_sum(terms)
    x, terms, label = call(
        middle_kernel,
        held(x.shape),
        spread_out,
        held(index.shape),
        scratch_shapes=[pltpu.VMEM((lanes, rows, LOW), jnp.bfloat16)],
    )(
        *in_vmem(margins, hots, turned, index, x, *kept, marks)
    )
    margins = tables_to_sum(terms)
    x, sent = call(last_kernel, held(x.shape), held((near, 3, lanes, size)))(
        *in_vmem(margins, hots, turned, index, x, *kept, label)
    )
    came = exchanged(sent, NEAR)
    consensus, dual, sums = call(
        consensus_kernel, held(x.shape), held(x.shape), held((far, LANES))
    )(*in_vmem(came, place, x, dual))
    sums = exchanged(sums.reshape(far, 1, LANES), FAR).reshape(far, LANES)
    whole = jax.ShapeDtypeStruct(x.shape, jnp.float32)
    x, dual, consensus, norms = call(
        finish_kernel,
        whole,
        whole,
        whole,
        jax.ShapeDtypeStruct((2,), jnp.float32),
        out_specs=(HBM, HBM, HBM, HBM),
        scratch_shapes=[pltpu.VMEM((2,), jnp.float32), pltpu.SemaphoreType.DMA((4,))],
    )(*in_vmem(sums, x, dual, consensus))
    return (x[None], dual[None], consensus, norms)


def solution(mesh):
    feat = {64: (8, 2, 2, 2), 16: (2, 2, 2, 2), 2: (1, 1, 1, 2)}[mesh.shape["feat"]]
    torus = Mesh(
        mesh.devices.reshape(*feat, mesh.shape["row"], mesh.shape["col"]), FEAT + SHARD
    )
    placed = (
        P(SHARD, FEAT, None),
        P(SHARD, FEAT, None),
        P(FEAT, None),
        P(SHARD, FEAT, None, None),
        P(SHARD, FEAT, None),
        P(SHARD, None),
    )
    return jax.shard_map(
        local,
        mesh=torus,
        in_specs=placed,
        out_specs=(P(SHARD, FEAT, None), P(SHARD, FEAT, None), P(FEAT, None), P()),
        check_vma=False,
    )
```
